32 devices in a mesh: dp: 2 (over core), seq: 4 (over y, x), tensor: 4 (over z).
Axes of the slice: x: 2, y: 2, z: 4, core: 2. Of those that a mesh axis runs over, the one named last changes fastest.
Arguments:
- tokens: bfloat16 [2, 2048, 2048], P('dp', ('seq', 'tensor')), may hold values from -6 to 6
- attn_gain: float32 [2048], replicated, may hold values from 0.5 to 1.5
- w_qkv: bfloat16 [3, 2048, 2048], P(None, None, 'tensor'), may hold values from -1 to 1
- w_out: bfloat16 [2048, 2048], P('tensor'), may hold values from -0.125 to 0.125
- mlp_gain: float32 [2048], replicated, may hold values from 0.5 to 1.5
- w_up: bfloat16 [2048, 8192], P(None, 'tensor'), may hold values from -0.125 to 0.125
- w_down: bfloat16 [8192, 2048], P('tensor'), may hold values from -0.0625 to 0.0625
- pool_gain: float32 [2048], replicated, may hold values from -8 to 8
- pool_bias: float32 [2048], replicated, may hold values from 0.5 to 5
- value_weight: float32 [2048], replicated, may hold values from -6 to 6
- valid_frames: int32 [2], replicated, may hold values from 4 to 8, as said below
Outputs:
- hidden: bfloat16 [2, 2048, 2048], P('dp', ('seq', 'tensor'))
- frame_values: float32 [2, 8], P('dp', 'seq')
- advantages: float32 [2, 8], P('dp', 'seq')
The draws below stay inside these ranges and needn't reach their ends.
Inputs may be any that keep to these rules, and one draw needn't show every extreme that they name: `valid_frames`: at least one rollout keeps all 8 frames and at least one keeps 8 // 2 of them.
All inputs are finite; a program needn't handle non-finite values.
Results may differ from the reference program's by a relative error of at most 0.017.
Values may be sent and summed in bfloat16 or wider, within the bound.
A program may use at most 256 MiB of HBM per device.

```python
import jax
import jax.numpy as jnp
from jax import lax

D = 2048
HEADS = 16
HEAD_DIM = 128
FF = 8192
TOK_FRAME = 256
FRAMES = 8
TOKENS = 2048
ROLLOUTS = 2


def draw_tokens(key, part):
    noise_key = jax.random.fold_in(key, 11)
    values = jax.random.truncated_normal(noise_key, -6.0, 6.0, (ROLLOUTS, TOKENS, D), jnp.float32)
    return values.astype(jnp.bfloat16)


def draw_w_qkv(key, part):
    base = jax.random.truncated_normal(jax.random.fold_in(key, 21), -6.0, 6.0, (3, D, D), jnp.float32) / jnp.sqrt(jnp.float32(D))
    return base.astype(jnp.bfloat16)


def draw_valid_frames(key, part):
    base = jax.random.randint(jax.random.fold_in(key, 31), (ROLLOUTS,), FRAMES // 2, FRAMES + 1, dtype=jnp.int32)
    rank = jax.random.permutation(jax.random.fold_in(key, 32), jnp.arange(ROLLOUTS, dtype=jnp.int32))
    longest = jnp.full((ROLLOUTS,), FRAMES, jnp.int32)
    shortest = jnp.full((ROLLOUTS,), FRAMES // 2, jnp.int32)
    return jnp.where(rank == 0, longest, jnp.where(rank == 1, shortest, base)).astype(jnp.int32)


def shard_levels(stream_key, shape, split, least, high):
    level = 1.0
    for dim, parts in split:
        heights = jax.random.uniform(jax.random.fold_in(jax.random.fold_in(stream_key, 6), dim), (parts,), jnp.float32, least / len(split), high / len(split))
        level = level * jnp.repeat(jnp.exp(heights), shape[dim] // parts).reshape((-1,) + (1,) * (len(shape) - 1 - dim))
    return level


def normal_values(rng, dims, scale, reach, shards=(), held_as=jnp.bfloat16):
    array = scale * jax.random.normal(rng, dims, jnp.float32)
    if shards:
        array = array * shard_levels(rng, dims, shards, -0.22, 0.18)
    return jnp.clip(array, -reach, reach).astype(held_as)


def setup_inputs(seed: int = 0) -> dict:
    key_list = jax.random.split(jax.random.key(seed), 12)
    tokens = draw_tokens(jax.random.fold_in(key_list[11], 71), 0)
    attn_gain = jnp.clip(1.0 + 0.1 * jax.random.normal(key_list[1], (D,), jnp.float32), 0.5, 1.5)
    w_qkv = draw_w_qkv(jax.random.fold_in(key_list[11], 71), 0)
    w_out = normal_values(key_list[3], (D, D), D ** -0.5, 0.125, ((0, 4),))
    mlp_gain = jnp.clip(1.0 + 0.1 * jax.random.normal(key_list[4], (D,), jnp.float32), 0.5, 1.5)
    w_up = normal_values(key_list[5], (D, FF), D ** -0.5, 0.125, ((1, 4),))
    w_down = normal_values(key_list[6], (FF, D), FF ** -0.5, 0.0625, ((0, 4),))
    pool_gain = jnp.clip(jax.random.uniform(key_list[7], (D,), jnp.float32, -8.0, 8.0), -8.0, 8.0)
    pool_bias = jnp.clip(jax.random.uniform(key_list[8], (D,), jnp.float32, 0.5, 5.0), 0.5, 5.0)
    value_weight = normal_values(key_list[9], (D,), 1.0, 6.0, (), jnp.float32)
    valid_frames = draw_valid_frames(jax.random.fold_in(key_list[11], 71), 0)
    return dict(tokens=tokens, attn_gain=attn_gain, w_qkv=w_qkv, w_out=w_out, mlp_gain=mlp_gain, w_up=w_up, w_down=w_down, pool_gain=pool_gain, pool_bias=pool_bias, value_weight=value_weight, valid_frames=valid_frames)


def rms_norm(values, gain):
    floats = values.astype(jnp.float32)
    square = lax.optimization_barrier(jnp.mean(floats * floats, axis=-1, keepdims=True))
    return (floats * lax.rsqrt(square + 1e-05) * gain).astype(jnp.bfloat16)

def reference(tokens, attn_gain, w_qkv, w_out, mlp_gain, w_up, w_down, pool_gain, pool_bias, value_weight, valid_frames):
    scale = 1.0 / HEAD_DIM ** 0.5
    frame_of = jnp.arange(TOKENS, dtype=jnp.int32) // TOK_FRAME

    def layer(args):
        rows, length = args
        normed = rms_norm(rows, attn_gain)
        qkv = jnp.einsum('nd,cde->nce', normed.astype(jnp.float32), w_qkv.astype(jnp.float32)).astype(jnp.bfloat16)
        query = qkv[:, 0].reshape(TOKENS, HEADS, HEAD_DIM).transpose(1, 0, 2)
        keys = qkv[:, 1].reshape(TOKENS, HEADS, HEAD_DIM).transpose(1, 0, 2)
        vals = qkv[:, 2].reshape(TOKENS, HEADS, HEAD_DIM).transpose(1, 0, 2)
        allowed = (frame_of[None, :] <= frame_of[:, None]) & (frame_of[None, :] < length)

        def head(trio):
            qh, kh, vh = trio
            scores = jnp.dot(qh, kh.T, preferred_element_type=jnp.float32) * scale
            scores = jnp.where(allowed, scores, -1e+30)
            peak = lax.optimization_barrier(jnp.max(scores, axis=-1, keepdims=True))
            weights = jnp.where(allowed, jnp.exp(scores - peak), 0.0)
            total = lax.optimization_barrier(jnp.sum(weights, axis=-1, keepdims=True))
            numer = jnp.dot(weights.astype(jnp.bfloat16), vh, preferred_element_type=jnp.float32)
            return numer / total
        mixed = lax.map(head, (query, keys, vals)).transpose(1, 0, 2).reshape(TOKENS, D).astype(jnp.bfloat16)
        after_attn = (rows.astype(jnp.float32) + jnp.dot(mixed, w_out, preferred_element_type=jnp.float32)).astype(jnp.bfloat16)
        normed2 = rms_norm(after_attn, mlp_gain)
        up = jax.nn.gelu(jnp.dot(normed2, w_up, preferred_element_type=jnp.float32), approximate=True).astype(jnp.bfloat16)
        return (after_attn.astype(jnp.float32) + jnp.dot(up, w_down, preferred_element_type=jnp.float32)).astype(jnp.bfloat16)
    hidden = lax.map(layer, (tokens, valid_frames))
    means = lax.optimization_barrier(jnp.mean(hidden.astype(jnp.float32).reshape(ROLLOUTS, FRAMES, TOK_FRAME, D), axis=2))
    frame_ids = jnp.arange(FRAMES, dtype=jnp.int32)
    valid = frame_ids[None, :] < valid_frames[:, None]

    def advance(state, inputs):
        mean_f, valid_f = inputs
        gate = jax.nn.sigmoid(mean_f * pool_gain + pool_bias)
        new = gate * state + (1.0 - gate) * mean_f
        state = jnp.where(valid_f[:, None], new, state)
        return (state, state)
    start = jnp.zeros((ROLLOUTS, D), jnp.float32)
    _, states = lax.scan(advance, start, (means.transpose(1, 0, 2), valid.T))
    states = states.transpose(1, 0, 2)
    frame_values = jnp.where(valid, lax.optimization_barrier(jnp.sum(states * value_weight, axis=-1)), 0.0)
    last = frame_ids[None, :] == valid_frames[:, None] - 1
    reward = lax.optimization_barrier(jnp.sum(jnp.where(last, frame_values, 0.0), axis=1))
    gap = jnp.where(valid, reward[:, None] - frame_values, 0.0)
    count = jnp.sum(valid_frames).astype(jnp.float32)
    mean = jnp.sum(gap) / count
    centered = jnp.where(valid, gap - mean, 0.0)
    variance = jnp.sum(centered * centered) / count
    advantages = jnp.where(valid, centered * lax.rsqrt(variance + 1e-05), 0.0)
    return (hidden, frame_values, advantages)
```

```python
import math

import jax
import jax.numpy as jnp
from jax import lax
from jax.experimental import pallas as pl
from jax.experimental.pallas import tpu as pltpu
from jax.sharding import PartitionSpec as P

HEAD_DIM = 128
TOK_FRAME = 256
LANES = 128
CHUNKS = 4
HALVES = 2
LAG = 2
MESH = pl.DeviceIdType.MESH
F32 = jnp.float32
BF16 = jnp.bfloat16


def rms_norm(floats, gain):
    square = jnp.mean(floats * floats, axis=-1, keepdims=True)
    return (floats * lax.rsqrt(square + 1e-05) * gain).astype(BF16)


def loop(n, body):
    def step(i, carry):
        body(i)
        return carry

    lax.fori_loop(0, n, step, 0)


def kernel(
    tok, attn_gain, w_qkv_h, w_out_h, mlp_gain, w_up_h, w_down_h, pool_gain, pool_bias,
    value_weight, lens,
    hidden, small,
    w_qkv, w_out, w_up, w_down, ag1, query, kv, peak, total, acc, mixed, aft, own, normed,
    upbuf, part, rs, fsum, means,
    wsem, ag_s, ag_r, kv_s, kv_r, kvr_s, wz_s, wp_s, wr_s, wd_s, wo_r, mx_s, mx_r, rs_s, rs_r,
    fs_s, fs_r, mn_s, mn_r,
):
    T, S, DP = (lax.axis_size("tensor"), lax.axis_size("seq"), lax.axis_size("dp"))
    z, me, roll = (lax.axis_index("tensor"), lax.axis_index("seq"), lax.axis_index("dp"))
    C, cr, width = tok.shape
    rows = C * cr
    block = rows * T
    qc = T * cr
    NH = HALVES
    per_half = C // NH
    hr = rows // NH
    hcols = query.shape[-1]
    heads = hcols // HEAD_DIM
    ff = w_up.shape[1]
    fr_dev = block // TOK_FRAME
    square = S == 4
    right, left = (lax.rem(z + 1, T), lax.rem(z + T - 1, T))
    tile = 1024
    ends = (z == 0) | (z == T - 1)
    mine = roll * S + me
    other = lax.rem(roll + 1, DP)

    loads = [
        pltpu.make_async_copy(src, dst, wsem.at[i])
        for i, (src, dst) in enumerate(
            ((w_qkv_h, w_qkv), (w_out_h, w_out.at[z]), (w_up_h, w_up), (w_down_h, w_down))
        )
    ]
    for load in loads:
        load.start()

    barrier = pltpu.get_barrier_semaphore()
    for d in range(1, T):
        pl.semaphore_signal(barrier, 1, device_id={"tensor": lax.rem(z + d, T)}, device_id_type=MESH)
    peers = []
    for a in range(DP):
        for b in range(S):
            if a or b:
                peers.append({"dp": lax.rem(roll + a, DP), "seq": lax.rem(me + b, S)})
    for peer in peers:
        pl.semaphore_signal(barrier, 1, device_id=peer, device_id_type=MESH)
    pl.semaphore_wait(barrier, T - 1 + len(peers))

    def rcopy(src, dst, s_sem, r_sem, to):
        return pltpu.make_async_remote_copy(
            src_ref=src, dst_ref=dst, send_sem=s_sem, recv_sem=r_sem, device_id=to,
            device_id_type=MESH,
        )

    def zcopy(src, dst, s_sem, r_sem, to):
        return rcopy(src, dst, s_sem, r_sem, {"tensor": to})

    def toward(way):
        return right if way == 0 else left

    def tok_send(s, h, way, src=None):
        ref = ag1.at[s, pl.ds(h * per_half, per_half)]
        return zcopy(ref if src is None else src, ref, ag_s.at[way, s, h], ag_r.at[s, h], toward(way))

    def own_send(h, way):
        return tok_send(z, h, way, tok.at[pl.ds(h * per_half, per_half)])

    for h in range(NH):

        @pl.when(z < T - 1)
        def _(h=h):
            own_send(h, 0).start()

        @pl.when(z > 0)
        def _(h=h):
            own_send(h, 1).start()

    def arrival(u):
        near = jnp.minimum(z, T - 1 - z)
        paired = u <= 2 * near
        k = jnp.where(paired, lax.div(u + 1, 2), u - near)
        odd = lax.rem(u, 2)
        longer = jnp.where(z > T - 1 - z, 1, 0)
        from_left = jnp.where(paired, odd, longer)
        return (jnp.where(from_left == 1, z - k, z + k), from_left)

    def kv_copy(j, s, h, i, sem, to):
        ref = kv.at[j, s, h, i]
        return rcopy(ref, ref, sem, kv_r.at[j, s, h, i], {"seq": to})

    def kv_send(d, s, h, i):
        return kv_copy(me, s, h, i, kv_s.at[d, s, h, i], lax.rem(me + d, S))

    def kv_direct(d):
        cond = me + d < S
        if square and d == 3:
            cond = cond & (me != 0)
        if square and d == 1:
            cond = cond & (me != 1)
        return cond

    relay_from = jnp.where(me == 3, 1, 0)
    relay_to = jnp.where(me == 3, 2, 3)

    def relays(i):
        return (me == 3) | (me == 1 + i)

    def kv_relay_copy(s, h, i):
        return kv_copy(relay_from, s, h, i, kvr_s.at[s, h, i], relay_to)

    def kv_relay(n):
        if square:
            s, _ = arrival(lax.div(n, NH))
            h = lax.rem(n, NH)
            for i in range(2):

                @pl.when(relays(i))
                def _(i=i):
                    copy = kv_relay_copy(s, h, i)
                    copy.wait_recv()
                    copy.start()

    def kv_rest(n):
        s, h = (lax.div(n, NH), lax.rem(n, NH))

        def source(j, carry):
            for i in range(2):
                cond = j < me
                if square:
                    cond = cond & jnp.logical_not(relays(i) & (j == relay_from))

                @pl.when(cond)
                def _(i=i):
                    kv_copy(j, s, h, i, kv_s.at[0, s, h, i], lax.rem(me + 1, S)).wait_recv()

            return carry

        lax.fori_loop(0, S - 1, source, 0)

    def project(s, h):
        floats = ag1[s, pl.ds(h * per_half, per_half)].astype(F32).reshape(hr, width)
        x = rms_norm(floats, attn_gain[...])
        for i in range(2):
            kv[me, s, h, i] = jnp.dot(x, w_qkv[1 + i], preferred_element_type=F32).astype(BF16)
            for d in range(1, S):

                @pl.when(kv_direct(d))
                def _(d=d, i=i):
                    kv_send(d, s, h, i).start()

        q = jnp.dot(x, w_qkv[0], preferred_element_type=F32).astype(BF16)
        query[s, pl.ds(h * per_half, per_half)] = q.reshape(per_half, cr, hcols)

    def w_ref(zz, r, f):
        half = w_out.shape[2] // 2
        return w_out.at[zz, r, pl.ds(f * half, half)]

    def w_copy(zz, r, f, sem, to):
        ref = w_ref(zz, r, f)
        return rcopy(ref, ref, sem, wo_r.at[zz, r, f], to)

    def wz_send(zz, f, way):
        return w_copy(zz, mine, f, wz_s.at[way, zz, f], {"tensor": toward(way)})

    flip_x = me + 1 - 2 * lax.rem(me, 2)
    flip_y = lax.rem(me + 2, 4)
    flip_d = flip_x + 2 - 4 * lax.div(flip_x, 2)

    def plane_targets():
        if square:
            return [flip_x, flip_y]
        return [lax.rem(me + d, S) for d in range(1, S)]

    def plane_sends(zz, f):
        return [
            w_copy(zz, mine, f, wp_s.at[n, zz, f], {"seq": to})
            for n, to in enumerate(plane_targets())
        ]

    def die_send(zz, b, f):
        return w_copy(zz, roll * S + b, f, wd_s.at[b, zz, f], {"dp": other})

    def w_relay(zz, axis):
        if axis == 0:
            return w_copy(zz, roll * S + flip_x, 0, wr_s.at[zz, 0], {"seq": flip_y})
        return w_copy(zz, roll * S + flip_y, 1, wr_s.at[zz, 1], {"seq": flip_x})

    def w_begin():
        for f in range(2):

            @pl.when(z < T - 1)
            def _(f=f):
                wz_send(z, f, 0).start()

            @pl.when(z > 0)
            def _(f=f):
                wz_send(z, f, 1).start()

    def sides(k):
        return ((z - k, z - k >= 0, 0, z < T - 1), (z + k, z + k < T, 1, z > 0))

    def w_step(k):
        for zz, here, way, more in sides(k):

            @pl.when(here)
            def _(zz=zz, way=way, more=more):
                for f in range(2):
                    wz_send(zz, f, way).wait_recv()

                    @pl.when(more)
                    def _(f=f):
                        wz_send(zz, f, way).start()

                    for copy in plane_sends(zz, f):
                        copy.start()
                    die_send(zz, me, f).start()

    def w_spread(k):
        for zz, here, _, _ in sides(k):

            @pl.when(here)
            def _(zz=zz):
                if square:
                    for axis, b in ((0, flip_x), (1, flip_y)):
                        for f in range(2):
                            die_send(zz, b, f).wait_recv()
                        w_relay(zz, axis).start()
                        for f in range(2):
                            die_send(zz, b, f).start()
                else:
                    for d in range(1, S):
                        b = lax.rem(me + d, S)
                        for f in range(2):
                            die_send(zz, b, f).wait_recv()
                            die_send(zz, b, f).start()

    def w_diagonal(k):
        if square:
            for zz, here, _, _ in sides(k):

                @pl.when(here)
                def _(zz=zz):
                    for f in range(2):
                        copy = die_send(zz, flip_d, f)
                        copy.wait_recv()
                        copy.start()

    def w_finish(k):
        for zz, here, _, _ in sides(k):

            @pl.when(here)
            def _(zz=zz):
                def piece(b, carry):
                    for f in range(2):
                        w_copy(
                            zz, other * S + b, f, wd_s.at[b, zz, f], {"dp": other}
                        ).wait_recv()
                    return carry

                lax.fori_loop(0, S, piece, 0)

    def w_drain(k):
        for zz, here, way, more in sides(k):

            @pl.when(here)
            def _(zz=zz, way=way, more=more):
                for f in range(2):

                    @pl.when(more)
                    def _(f=f):
                        wz_send(zz, f, way).wait_send()

                    for copy in plane_sends(zz, f):
                        copy.wait_send()
                    if square:
                        w_relay(zz, f).wait_send()

                def piece(b, carry):
                    for f in range(2):
                        die_send(zz, b, f).wait_send()
                    return carry

                lax.fori_loop(0, S, piece, 0)

    ag1[z] = tok[...]
    loads[0].wait()

    def gather(i):
        u, h = (lax.div(i, NH), lax.rem(i, NH))
        s, from_left = arrival(u)

        @pl.when(u > 0)
        def _():
            tok_send(s, h, 0).wait_recv()

            @pl.when((from_left == 1) & (z < T - 1))
            def _():
                tok_send(s, h, 0).start()

            @pl.when((from_left == 0) & (z > 0))
            def _():
                tok_send(s, h, 1).start()

        @pl.when(i == NH)
        def _():
            loads[1].wait()

            @pl.when(ends)
            def _():
                w_begin()

        project(s, h)

        @pl.when(i >= LAG)
        def _():
            kv_relay(i - LAG)

    loop(T * NH, gather)

    @pl.when(jnp.logical_not(ends))
    def _():
        w_begin()

    length = lens[pl.ds(roll, 1)][0, 0:1, 0:1].astype(jnp.int32)
    to_bits = math.log2(math.e) / HEAD_DIM**0.5

    def attend(c):
        peak[...] = jnp.full_like(peak, -1e30)
        total[...] = jnp.zeros_like(total)
        acc[...] = jnp.zeros_like(acc)
        q_row = lax.div(lax.broadcasted_iota(jnp.int32, (fr_dev, 1, qc), 2), cr) * rows
        q_frame = me * fr_dev + lax.div(q_row, TOK_FRAME)
        k_local = lax.broadcasted_iota(jnp.int32, (fr_dev, 1, qc), 0)

        def against(j, carry):
            k_frame = j * fr_dev + k_local
            bias = jnp.where((k_frame <= q_frame) & (k_frame < length), 0.0, -1e30)
            for h in range(heads):
                cols = slice(h * HEAD_DIM, (h + 1) * HEAD_DIM)
                q = query[:, c, :, cols].reshape(qc, HEAD_DIM)
                k = kv[j, :, :, 0, :, cols].reshape(block, HEAD_DIM)
                v = kv[j, :, :, 1, :, cols].reshape(block, HEAD_DIM)
                s = lax.dot_general(k, q, (((1,), (1,)), ((), ())), preferred_element_type=F32)
                s = s.reshape(fr_dev, TOK_FRAME, qc) * to_bits + bias
                s = s.reshape(block, qc)
                old = peak[h]
                new = jnp.maximum(old, jnp.max(s, axis=0, keepdims=True))
                weights = jnp.exp2(s - new)
                shrink = jnp.exp2(old - new)
                peak[h] = new
                total[h] = total[h] * shrink + jnp.sum(weights, axis=0, keepdims=True)
                acc[h] = acc[h] * shrink + lax.dot_general(
                    v, weights.astype(BF16), (((0,), (0,)), ((), ())), preferred_element_type=F32
                )
            return carry

        lax.fori_loop(0, me + 1, against, 0)
        for h in range(heads):
            cols = slice(h * HEAD_DIM, (h + 1) * HEAD_DIM)
            mixed[c, z, :, cols] = jnp.transpose(acc[h] / total[h]).astype(BF16)

    def mx_send(c, s, way):
        ref = mixed.at[c, s]
        return zcopy(ref, ref, mx_s.at[way, c, s], mx_r.at[c, s], toward(way))

    def mx_begin(c):
        @pl.when(z < T - 1)
        def _():
            mx_send(c, z, 0).start()

        @pl.when(z > 0)
        def _():
            mx_send(c, z, 1).start()

    def mx_step(c, k):
        for s, here, way, more in sides(k):

            @pl.when(here)
            def _(s=s, way=way, more=more):
                copy = mx_send(c, s, way)
                copy.wait_recv()

                @pl.when(more)
                def _():
                    copy.start()

    def rs_send(c, d, way, opens):
        src = part.at[c, d] if opens else rs.at[c, way, d]
        return zcopy(src, rs.at[c, way, d], rs_s.at[way, c, d], rs_r.at[way, c, d], toward(way))

    def rs_open(c):
        for i in range(T - 1):

            @pl.when((z == 0) & (T - 1 - i > z))
            def _(i=i):
                rs_send(c, T - 1 - i, 0, True).start()

            @pl.when((z == T - 1) & (i < z))
            def _(i=i):
                rs_send(c, i, 1, True).start()

    def rs_pass(c, w, i):
        for d, way, here in (
            (T - 1 - i, 0, (z == w) & (T - 1 - i > z)),
            (i, 1, (T - 1 - z == w) & (i < z)),
        ):

            @pl.when(here)
            def _(d=d, way=way):
                copy = rs_send(c, d, way, False)
                copy.wait_recv()
                rs[c, way, d] = (rs[c, way, d].astype(F32) + part[c, d].astype(F32)).astype(BF16)
                copy.start()

    def rs_finish(c):
        own[c] = own[c] + part[c, z].astype(F32)

        @pl.when(z > 0)
        def _():
            rs_send(c, z, 0, False).wait_recv()
            own[c] = own[c] + rs[c, 0, z].astype(F32)

        @pl.when(z < T - 1)
        def _():
            rs_send(c, z, 1, False).wait_recv()
            own[c] = own[c] + rs[c, 1, z].astype(F32)

        hidden[c] = own[c].astype(BF16)

    passes = [(w, i) for w in range(1, T - 1) for i in range(T - 1 - w)]

    def project_out(c):
        lhs = jnp.concatenate([mixed[c, s] for s in range(T)], axis=1)

        def cols_of(n):
            cols = pl.ds(pl.multiple_of(n * tile, tile), tile)
            w = w_out[:, :, :, cols].reshape(T * hcols, tile)
            res = jnp.dot(lhs, w, preferred_element_type=F32)
            res = res + ag1[:, c, :, cols].astype(F32).reshape(qc, tile)
            aft[:, :, cols] = res.astype(BF16).reshape(T, cr, tile)

        loop(width // tile, cols_of)
        normed[...] = rms_norm(aft[...].astype(F32).reshape(qc, width), mlp_gain[...])
        own[c] = aft[z].astype(F32)

    def feed_up():
        def cols_of(n):
            cols = pl.ds(pl.multiple_of(n * tile, tile), tile)
            res = jnp.dot(normed[...], w_up[:, cols], preferred_element_type=F32)
            upbuf[:, cols] = jax.nn.gelu(res, approximate=True).astype(BF16)

        loop(ff // tile, cols_of)

    def feed_down(c):
        def cols_of(n):
            cols = pl.ds(pl.multiple_of(n * tile, tile), tile)
            res = jnp.dot(upbuf[...], w_down[:, cols], preferred_element_type=F32)
            part[c, :, :, cols] = res.astype(BF16).reshape(T, cr, tile)

        loop(width // tile, cols_of)

    w_step(1)
    for n in range(T * NH - LAG, T * NH):
        kv_relay(jnp.int32(n))
    loop(T * NH, kv_rest)
    w_step(2)

    def mix(c):
        attend(c)
        mx_begin(c)

        @pl.when(c == 0)
        def _():
            for k in range(3, T):
                w_step(k)

        @pl.when(c == 1)
        def _():
            w_spread(1)

        @pl.when(c == 2)
        def _():
            w_spread(2)
            w_diagonal(1)

    loop(C, mix)
    for k in range(3, T):
        w_spread(k)
    for k in range(2, T):
        w_diagonal(k)
    loads[2].wait()
    loads[3].wait()

    def chunk(c):
        for k in range(1, T):
            mx_step(c, k)
            for w, i in passes[k - 1 : k]:

                @pl.when(c > 0)
                def _(w=w, i=i):
                    rs_pass(c - 1, w, i)

        @pl.when(c == 0)
        def _():
            for k in range(1, T):
                w_finish(k)

        project_out(c)
        for w, i in passes[T - 1 :]:

            @pl.when(c > 0)
            def _(w=w, i=i):
                rs_pass(c - 1, w, i)

        feed_up()
        feed_down(c)
        rs_open(c)

        @pl.when(c > 0)
        def _():
            rs_finish(c - 1)

    loop(C, chunk)
    for w, i in passes:
        rs_pass(C - 1, w, i)
    rs_finish(C - 1)

    out = hidden[...].astype(F32).reshape(rows, width)
    sums = jnp.sum(out, axis=0, keepdims=True)
    chunks = width // LANES
    for c in range(chunks):
        fsum[z, c : c + 1, :] = sums[:, c * LANES : (c + 1) * LANES]

    def fs_send(d):
        return zcopy(fsum.at[z], fsum.at[z], fs_s.at[d], fs_r.at[z], lax.rem(z + d, T))

    for d in range(1, T):
        fs_send(d).start()
    for d in range(1, T):
        o = lax.rem(z + T - d, T)
        zcopy(fsum.at[o], fsum.at[o], fs_s.at[0], fs_r.at[o], right).wait_recv()
    per = T // fr_dev
    for f in range(fr_dev):
        m = fsum[f * per]
        for s in range(f * per + 1, (f + 1) * per):
            m = m + fsum[s]
        means[roll, me, f] = m / TOK_FRAME

    def mn_send(i, peer):
        return rcopy(means.at[roll, me], means.at[roll, me], mn_s.at[i], mn_r.at[roll, me], peer)

    for i, peer in enumerate(peers):
        mn_send(i, peer).start()
    for a in range(DP):
        for b in range(S):
            if a or b:
                ra, sb = (lax.rem(roll + a, DP), lax.rem(me + b, S))
                rcopy(
                    means.at[ra, sb], means.at[ra, sb], mn_s.at[0], mn_r.at[ra, sb], peers[0]
                ).wait_recv()

    lane = lax.broadcasted_iota(jnp.int32, (1, LANES), 1)
    values, gaps, valids = ([], [], [])
    for r in range(DP):
        span = lens[r]

        def frame(f, carry):
            state, vec = carry
            m = means[r, f // fr_dev, lax.rem(f, fr_dev)]
            gate = jax.nn.sigmoid(m * pool_gain[...] + pool_bias[...])
            new = gate * state + (1.0 - gate) * m
            state = jnp.where(span > f.astype(F32), new, state)
            dot = jnp.sum(jnp.sum(state * value_weight[...], axis=1, keepdims=True), axis=0, keepdims=True)
            return (state, jnp.where(lane == f, dot, vec))

        zero = (jnp.zeros((chunks, LANES), F32), jnp.zeros((1, LANES), F32))
        _, vec = lax.fori_loop(0, S * fr_dev, frame, zero)
        length_r = span[0:1].astype(jnp.int32)
        ok = lane < length_r
        vec = jnp.where(ok, vec, 0.0)
        reward = jnp.sum(jnp.where(lane == length_r - 1, vec, 0.0), axis=1, keepdims=True)
        values.append(vec)
        valids.append(ok)
        gaps.append(jnp.where(ok, reward - vec, 0.0))
    count = sum(lens[r][0:1, 0:1] for r in range(DP))
    mean = sum(jnp.sum(g, axis=1, keepdims=True) for g in gaps) / count
    centered = [jnp.where(ok, g - mean, 0.0) for ok, g in zip(valids, gaps)]
    variance = sum(jnp.sum(c * c, axis=1, keepdims=True) for c in centered) / count
    for r in range(DP):
        small[r : r + 1, :] = values[r]
        small[DP + r : DP + r + 1, :] = jnp.where(
            valids[r], centered[r] * lax.rsqrt(variance + 1e-05), 0.0
        )

    for h in range(NH):

        @pl.when(z < T - 1)
        def _(h=h):
            own_send(h, 0).wait_send()

        @pl.when(z > 0)
        def _(h=h):
            own_send(h, 1).wait_send()

    for k in range(1, T):
        for s, here, way, more in sides(k):

            @pl.when(here & more)
            def _(s=s, way=way):
                for h in range(NH):
                    tok_send(s, h, way).wait_send()

                def sent(c):
                    mx_send(c, s, way).wait_send()

                loop(C, sent)

        w_drain(k)
    for way, more in ((0, z < T - 1), (1, z > 0)):

        @pl.when(more)
        def _(way=way):
            for f in range(2):
                wz_send(z, f, way).wait_send()

            def sent(c):
                mx_send(c, z, way).wait_send()

            loop(C, sent)

    def rs_drain(c):
        for d in range(T):

            @pl.when(z < d)
            def _(d=d):
                rs_send(c, d, 0, False).wait_send()

            @pl.when(z > d)
            def _(d=d):
                rs_send(c, d, 1, False).wait_send()

    loop(C, rs_drain)

    def kv_drain(n):
        s, h = (lax.div(n, NH), lax.rem(n, NH))
        for i in range(2):
            for d in range(1, S):

                @pl.when(kv_direct(d))
                def _(d=d, i=i):
                    kv_send(d, s, h, i).wait_send()

            if square:

                @pl.when(relays(i))
                def _(i=i):
                    kv_relay_copy(s, h, i).wait_send()

    loop(T * NH, kv_drain)
    for d in range(1, T):
        fs_send(d).wait_send()
    for i, peer in enumerate(peers):
        mn_send(i, peer).wait_send()


def local(
    tokens, attn_gain, w_qkv, w_out, mlp_gain, w_up, w_down, pool_gain, pool_bias, value_weight,
    valid_frames,
):
    T, S, DP = (lax.axis_size("tensor"), lax.axis_size("seq"), lax.axis_size("dp"))
    rows, width = tokens.shape[1:]
    block = rows * T
    fr_dev = block // TOK_FRAME
    chunks = width // LANES
    hcols = w_qkv.shape[2]
    heads = hcols // HEAD_DIM
    C, NH = (CHUNKS, HALVES)
    cr = rows // C
    qc = T * cr
    NP = DP * S
    assert TOK_FRAME % rows == 0 and S * fr_dev <= LANES and DP == 2
    lens = jnp.broadcast_to(valid_frames.astype(F32)[:, None, None], (DP, chunks, LANES))
    vm = pl.BlockSpec(memory_space=pltpu.VMEM)
    hbm = pl.BlockSpec(memory_space=pl.ANY)
    dma = pltpu.SemaphoreType.DMA
    small_rows = -(-2 * DP // 8) * 8
    hidden, small = pl.pallas_call(
        kernel,
        out_shape=(
            jax.ShapeDtypeStruct((C, cr, width), BF16),
            jax.ShapeDtypeStruct((small_rows, LANES), F32),
        ),
        in_specs=[vm, vm, hbm, hbm, vm, hbm, hbm, vm, vm, vm, vm],
        out_specs=(vm, vm),
        scratch_shapes=[
            pltpu.VMEM(w_qkv.shape, BF16),
            pltpu.VMEM((T, NP, hcols // NP, width), BF16),
            pltpu.VMEM(w_up.shape, BF16),
            pltpu.VMEM(w_down.shape, BF16),
            pltpu.VMEM((T, C, cr, width), BF16),
            pltpu.VMEM((T, C, cr, hcols), BF16),
            pltpu.VMEM((S, T, NH, 2, rows // NH, hcols), BF16),
            pltpu.VMEM((heads, 1, qc), F32),
            pltpu.VMEM((heads, 1, qc), F32),
            pltpu.VMEM((heads, HEAD_DIM, qc), F32),
            pltpu.VMEM((C, T, qc, hcols), BF16),
            pltpu.VMEM((T, cr, width), BF16),
            pltpu.VMEM((C, cr, width), F32),
            pltpu.VMEM((qc, width), BF16),
            pltpu.VMEM((qc, w_up.shape[1]), BF16),
            pltpu.VMEM((C, T, cr, width), BF16),
            pltpu.VMEM((C, 2, T, cr, width), BF16),
            pltpu.VMEM((T, chunks, LANES), F32),
            pltpu.VMEM((DP, S, fr_dev, chunks, LANES), F32),
            dma((4,)),
            dma((2, T, NH)),
            dma((T, NH)),
            dma((S, T, NH, 2)),
            dma((S, T, NH, 2)),
            dma((T, NH, 2)),
            dma((2, T, 2)),
            dma((S, T, 2)),
            dma((T, 2)),
            dma((S, T, 2)),
            dma((T, NP, 2)),
            dma((2, C, T)),
            dma((C, T)),
            dma((2, C, T)),
            dma((2, C, T)),
            dma((T,)),
            dma((T,)),
            dma((DP * S,)),
            dma((DP, S)),
        ],
        compiler_params=pltpu.CompilerParams(
            collective_id=0, has_side_effects=True, vmem_limit_bytes=67043328
        ),
    )(
        tokens.reshape(C, cr, width),
        attn_gain[None],
        w_qkv,
        w_out.reshape(NP, hcols // NP, width),
        mlp_gain[None],
        w_up,
        w_down,
        pool_gain.reshape(chunks, LANES),
        pool_bias.reshape(chunks, LANES),
        value_weight.reshape(chunks, LANES),
        lens,
    )
    roll, seq = (lax.axis_index("dp"), lax.axis_index("seq"))
    values = lax.dynamic_slice(small, (roll, seq * fr_dev), (1, fr_dev))
    advantages = lax.dynamic_slice(small, (DP + roll, seq * fr_dev), (1, fr_dev))
    return (hidden.reshape(1, rows, width), values, advantages)


def solution(mesh):
    in_specs = (
        P("dp", ("seq", "tensor"), None),
        P(),
        P(None, None, "tensor"),
        P("tensor", None),
        P(),
        P(None, "tensor"),
        P("tensor", None),
        P(),
        P(),
        P(),
        P(),
    )
    out_specs = (P("dp", ("seq", "tensor"), None), P("dp", "seq"), P("dp", "seq"))
    return jax.shard_map(local, mesh=mesh, in_specs=in_specs, out_specs=out_specs, check_vma=False)
```

```python
import math

import jax
import jax.numpy as jnp
from jax import lax
from jax.experimental import pallas as pl
from jax.experimental.pallas import tpu as pltpu
from jax.sharding import PartitionSpec as P

HEAD_DIM = 128
TOK_FRAME = 256
LANES = 128
CHUNKS = 4
HALVES = 2
LAG = 2
GROUP = 4
MESH = pl.DeviceIdType.MESH
F32 = jnp.float32
BF16 = jnp.bfloat16


def rms_norm(floats, gain):
    square = jnp.mean(floats * floats, axis=-1, keepdims=True)
    return (floats * lax.rsqrt(square + 1e-05) * gain).astype(BF16)


def loop(n, body):
    def step(i, carry):
        body(i)
        return carry

    lax.fori_loop(0, n, step, 0)


def kernel(
    tok, attn_gain, w_qkv_h, w_out_h, mlp_gain, w_up_h, w_down_h, pool_gain, pool_bias,
    value_weight, lens,
    hidden, small,
    w_qkv, w_out, w_up, w_down, ag1, query, kv, peak, total, acc, mixed, aft, own, normed,
    upbuf, part, rs, fsum, means, dots,
    wsem, ag_s, ag_r, kv_s, kv_r, kvr_s, wz_s, wp_s, wr_s, wd_s, wo_r, mx_s, mx_r, rs_s, rs_r,
    fs_s, fs_r, mn_s, mn_r,
):
    T, S, DP = (lax.axis_size("tensor"), lax.axis_size("seq"), lax.axis_size("dp"))
    z, me, roll = (lax.axis_index("tensor"), lax.axis_index("seq"), lax.axis_index("dp"))
    C, cr, width = tok.shape
    rows = C * cr
    block = rows * T
    qc = T * cr
    NH = HALVES
    per_half = C // NH
    hr = rows // NH
    hcols = query.shape[-1]
    heads = hcols // HEAD_DIM
    ff = w_up.shape[1]
    fr_dev = block // TOK_FRAME
    square = S == 4
    right, left = (lax.rem(z + 1, T), lax.rem(z + T - 1, T))
    tile = 1024
    ends = (z == 0) | (z == T - 1)
    mine = roll * S + me
    other = lax.rem(roll + 1, DP)

    loads = [
        pltpu.make_async_copy(src, dst, wsem.at[i])
        for i, (src, dst) in enumerate(
            ((w_qkv_h, w_qkv), (w_out_h, w_out.at[z]), (w_up_h, w_up), (w_down_h, w_down))
        )
    ]
    for load in loads:
        load.start()

    barrier = pltpu.get_barrier_semaphore()
    for d in range(1, T):
        pl.semaphore_signal(barrier, 1, device_id={"tensor": lax.rem(z + d, T)}, device_id_type=MESH)
    peers = []
    for a in range(DP):
        for b in range(S):
            if a or b:
                peers.append({"dp": lax.rem(roll + a, DP), "seq": lax.rem(me + b, S)})
    for peer in peers:
        pl.semaphore_signal(barrier, 1, device_id=peer, device_id_type=MESH)
    pl.semaphore_wait(barrier, T - 1 + len(peers))

    def rcopy(src, dst, s_sem, r_sem, to):
        return pltpu.make_async_remote_copy(
            src_ref=src, dst_ref=dst, send_sem=s_sem, recv_sem=r_sem, device_id=to,
            device_id_type=MESH,
        )

    def zcopy(src, dst, s_sem, r_sem, to):
        return rcopy(src, dst, s_sem, r_sem, {"tensor": to})

    def toward(way):
        return right if way == 0 else left

    def tok_send(s, h, way, src=None):
        ref = ag1.at[s, pl.ds(h * per_half, per_half)]
        return zcopy(ref if src is None else src, ref, ag_s.at[way, s, h], ag_r.at[s, h], toward(way))

    def own_send(h, way):
        return tok_send(z, h, way, tok.at[pl.ds(h * per_half, per_half)])

    for h in range(NH):

        @pl.when(z < T - 1)
        def _(h=h):
            own_send(h, 0).start()

        @pl.when(z > 0)
        def _(h=h):
            own_send(h, 1).start()

    def arrival(u):
        near = jnp.minimum(z, T - 1 - z)
        paired = u <= 2 * near
        k = jnp.where(paired, lax.div(u + 1, 2), u - near)
        odd = lax.rem(u, 2)
        longer = jnp.where(z > T - 1 - z, 1, 0)
        from_left = jnp.where(paired, odd, longer)
        return (jnp.where(from_left == 1, z - k, z + k), from_left)

    def kv_copy(j, s, h, i, sem, to):
        ref = kv.at[j, s, h, i]
        return rcopy(ref, ref, sem, kv_r.at[j, s, h, i], {"seq": to})

    def kv_send(d, s, h, i):
        return kv_copy(me, s, h, i, kv_s.at[d, s, h, i], lax.rem(me + d, S))

    def kv_direct(d):
        cond = me + d < S
        if square and d == 3:
            cond = cond & (me != 0)
        if square and d == 1:
            cond = cond & (me != 1)
        return cond

    relay_from = jnp.where(me == 3, 1, 0)
    relay_to = jnp.where(me == 3, 2, 3)

    def relays(i):
        return (me == 3) | (me == 1 + i)

    def kv_relay_copy(s, h, i):
        return kv_copy(relay_from, s, h, i, kvr_s.at[s, h, i], relay_to)

    def kv_relay(n):
        if square:
            s, _ = arrival(lax.div(n, NH))
            h = lax.rem(n, NH)
            for i in range(2):

                @pl.when(relays(i))
                def _(i=i):
                    copy = kv_relay_copy(s, h, i)
                    copy.wait_recv()
                    copy.start()

    def kv_rest(n):
        s, h = (lax.div(n, NH), lax.rem(n, NH))

        def source(j, carry):
            for i in range(2):
                cond = j < me
                if square:
                    cond = cond & jnp.logical_not(relays(i) & (j == relay_from))

                @pl.when(cond)
                def _(i=i):
                    kv_copy(j, s, h, i, kv_s.at[0, s, h, i], lax.rem(me + 1, S)).wait_recv()

            return carry

        lax.fori_loop(0, S - 1, source, 0)

    def project(s, h):
        floats = ag1[s, pl.ds(h * per_half, per_half)].astype(F32).reshape(hr, width)
        x = rms_norm(floats, attn_gain[...])
        for i in range(2):
            kv[me, s, h, i] = jnp.dot(x, w_qkv[1 + i], preferred_element_type=F32).astype(BF16)
            for d in range(1, S):

                @pl.when(kv_direct(d))
                def _(d=d, i=i):
                    kv_send(d, s, h, i).start()

        q = jnp.dot(x, w_qkv[0], preferred_element_type=F32).astype(BF16)
        query[s, pl.ds(h * per_half, per_half)] = q.reshape(per_half, cr, hcols)

    def w_ref(zz, r, f):
        half = w_out.shape[2] // 2
        return w_out.at[zz, r, pl.ds(f * half, half)]

    def w_copy(zz, r, f, sem, to):
        ref = w_ref(zz, r, f)
        return rcopy(ref, ref, sem, wo_r.at[zz, r, f], to)

    def wz_send(zz, f, way):
        return w_copy(zz, mine, f, wz_s.at[way, zz, f], {"tensor": toward(way)})

    flip_x = me + 1 - 2 * lax.rem(me, 2)
    flip_y = lax.rem(me + 2, 4)
    flip_d = flip_x + 2 - 4 * lax.div(flip_x, 2)

    def plane_targets():
        if square:
            return [flip_x, flip_y]
        return [lax.rem(me + d, S) for d in range(1, S)]

    def plane_sends(zz, f):
        return [
            w_copy(zz, mine, f, wp_s.at[n, zz, f], {"seq": to})
            for n, to in enumerate(plane_targets())
        ]

    def die_send(zz, b, f):
        return w_copy(zz, roll * S + b, f, wd_s.at[b, zz, f], {"dp": other})

    def w_relay(zz, axis):
        if axis == 0:
            return w_copy(zz, roll * S + flip_x, 0, wr_s.at[zz, 0], {"seq": flip_y})
        return w_copy(zz, roll * S + flip_y, 1, wr_s.at[zz, 1], {"seq": flip_x})

    def w_begin():
        for f in range(2):

            @pl.when(z < T - 1)
            def _(f=f):
                wz_send(z, f, 0).start()

            @pl.when(z > 0)
            def _(f=f):
                wz_send(z, f, 1).start()

    def sides(k):
        return ((z - k, z - k >= 0, 0, z < T - 1), (z + k, z + k < T, 1, z > 0))

    def w_step(k):
        for zz, here, way, more in sides(k):

            @pl.when(here)
            def _(zz=zz, way=way, more=more):
                for f in range(2):
                    wz_send(zz, f, way).wait_recv()

                    @pl.when(more)
                    def _(f=f):
                        wz_send(zz, f, way).start()

                    for copy in plane_sends(zz, f):
                        copy.start()
                    die_send(zz, me, f).start()

    def w_spread(k):
        for zz, here, _, _ in sides(k):

            @pl.when(here)
            def _(zz=zz):
                if square:
                    for axis, b in ((0, flip_x), (1, flip_y)):
                        for f in range(2):
                            die_send(zz, b, f).wait_recv()
                        w_relay(zz, axis).start()
                        for f in range(2):
                            die_send(zz, b, f).start()
                else:
                    for d in range(1, S):
                        b = lax.rem(me + d, S)
                        for f in range(2):
                            die_send(zz, b, f).wait_recv()
                            die_send(zz, b, f).start()

    def w_diagonal(k):
        if square:
            for zz, here, _, _ in sides(k):

                @pl.when(here)
                def _(zz=zz):
                    for f in range(2):
                        copy = die_send(zz, flip_d, f)
                        copy.wait_recv()
                        copy.start()

    def w_finish(k):
        for zz, here, _, _ in sides(k):

            @pl.when(here)
            def _(zz=zz):
                def piece(b, carry):
                    for f in range(2):
                        w_copy(
                            zz, other * S + b, f, wd_s.at[b, zz, f], {"dp": other}
                        ).wait_recv()
                    return carry

                lax.fori_loop(0, S, piece, 0)

    def w_drain(k):
        for zz, here, way, more in sides(k):

            @pl.when(here)
            def _(zz=zz, way=way, more=more):
                for f in range(2):

                    @pl.when(more)
                    def _(f=f):
                        wz_send(zz, f, way).wait_send()

                    for copy in plane_sends(zz, f):
                        copy.wait_send()
                    if square:
                        w_relay(zz, f).wait_send()

                def piece(b, carry):
                    for f in range(2):
                        die_send(zz, b, f).wait_send()
                    return carry

                lax.fori_loop(0, S, piece, 0)

    ag1[z] = tok[...]
    loads[0].wait()

    def gather(i):
        u, h = (lax.div(i, NH), lax.rem(i, NH))
        s, from_left = arrival(u)

        @pl.when(u > 0)
        def _():
            tok_send(s, h, 0).wait_recv()

            @pl.when((from_left == 1) & (z < T - 1))
            def _():
                tok_send(s, h, 0).start()

            @pl.when((from_left == 0) & (z > 0))
            def _():
                tok_send(s, h, 1).start()

        @pl.when(i == NH)
        def _():
            loads[1].wait()

            @pl.when(ends)
            def _():
                w_begin()

        project(s, h)

        @pl.when(i >= LAG)
        def _():
            kv_relay(i - LAG)

    loop(T * NH, gather)

    @pl.when(jnp.logical_not(ends))
    def _():
        w_begin()

    length = lens[roll]
    to_bits = math.log2(math.e) / HEAD_DIM**0.5

    def attend(c):
        peak[...] = jnp.full_like(peak, -1e30)
        total[...] = jnp.zeros_like(total)
        acc[...] = jnp.zeros_like(acc)
        q_row = lax.div(lax.broadcasted_iota(jnp.int32, (fr_dev, 1, qc), 2), cr) * rows
        q_frame = me * fr_dev + lax.div(q_row, TOK_FRAME)
        k_local = lax.broadcasted_iota(jnp.int32, (fr_dev, 1, qc), 0)

        def against(first, count):
            biases = []
            for j in range(count):
                k_frame = (first + j) * fr_dev + k_local
                biases.append(jnp.where((k_frame <= q_frame) & (k_frame < length), 0.0, -1e30))
            for h in range(heads):
                cols = slice(h * HEAD_DIM, (h + 1) * HEAD_DIM)
                q = query[:, c, :, cols].reshape(qc, HEAD_DIM)
                old, norm, out = (peak[h], total[h], acc[h])
                for j in range(count):
                    k = kv[first + j, :, :, 0, :, cols].reshape(block, HEAD_DIM)
                    v = kv[first + j, :, :, 1, :, cols].reshape(block, HEAD_DIM)
                    s = lax.dot_general(k, q, (((1,), (1,)), ((), ())), preferred_element_type=F32)
                    s = s.reshape(fr_dev, TOK_FRAME, qc) * to_bits + biases[j]
                    s = s.reshape(block, qc)
                    new = jnp.maximum(old, jnp.max(s, axis=0, keepdims=True))
                    weights = jnp.exp2(s - new)
                    shrink = jnp.exp2(old - new)
                    old = new
                    norm = norm * shrink + jnp.sum(weights, axis=0, keepdims=True)
                    out = out * shrink + lax.dot_general(
                        v, weights.astype(BF16), (((0,), (0,)), ((), ())), preferred_element_type=F32
                    )
                peak[h], total[h], acc[h] = (old, norm, out)

        loop(lax.div(me + 1, GROUP), lambda g: against(g * GROUP, GROUP))
        for count in range(1, GROUP):

            @pl.when(lax.rem(me + 1, GROUP) == count)
            def _(count=count):
                against(me + 1 - count, count)

        for h in range(heads):
            cols = slice(h * HEAD_DIM, (h + 1) * HEAD_DIM)
            mixed[c, z, :, cols] = jnp.transpose(acc[h] / total[h]).astype(BF16)

    def mx_send(c, s, way):
        ref = mixed.at[c, s]
        return zcopy(ref, ref, mx_s.at[way, c, s], mx_r.at[c, s], toward(way))

    def mx_begin(c):
        @pl.when(z < T - 1)
        def _():
            mx_send(c, z, 0).start()

        @pl.when(z > 0)
        def _():
            mx_send(c, z, 1).start()

    def mx_step(c, k):
        for s, here, way, more in sides(k):

            @pl.when(here)
            def _(s=s, way=way, more=more):
                copy = mx_send(c, s, way)
                copy.wait_recv()

                @pl.when(more)
                def _():
                    copy.start()

    def rs_send(c, d, way, opens):
        src = part.at[c, d] if opens else rs.at[c, way, d]
        return zcopy(src, rs.at[c, way, d], rs_s.at[way, c, d], rs_r.at[way, c, d], toward(way))

    def rs_open(c):
        for i in range(T - 1):

            @pl.when((z == 0) & (T - 1 - i > z))
            def _(i=i):
                rs_send(c, T - 1 - i, 0, True).start()

            @pl.when((z == T - 1) & (i < z))
            def _(i=i):
                rs_send(c, i, 1, True).start()

    def rs_pass(c, w, i):
        for d, way, here in (
            (T - 1 - i, 0, (z == w) & (T - 1 - i > z)),
            (i, 1, (T - 1 - z == w) & (i < z)),
        ):

            @pl.when(here)
            def _(d=d, way=way):
                copy = rs_send(c, d, way, False)
                copy.wait_recv()
                rs[c, way, d] = (rs[c, way, d].astype(F32) + part[c, d].astype(F32)).astype(BF16)
                copy.start()

    def rs_finish(c):
        own[c] = own[c] + part[c, z].astype(F32)

        @pl.when(z > 0)
        def _():
            rs_send(c, z, 0, False).wait_recv()
            own[c] = own[c] + rs[c, 0, z].astype(F32)

        @pl.when(z < T - 1)
        def _():
            rs_send(c, z, 1, False).wait_recv()
            own[c] = own[c] + rs[c, 1, z].astype(F32)

        hidden[c] = own[c].astype(BF16)

    passes = [(w, i) for w in range(1, T - 1) for i in range(T - 1 - w)]

    def project_out(c):
        lhs = jnp.concatenate([mixed[c, s] for s in range(T)], axis=1)

        def cols_of(n):
            cols = pl.ds(pl.multiple_of(n * tile, tile), tile)
            w = w_out[:, :, :, cols].reshape(T * hcols, tile)
            res = jnp.dot(lhs, w, preferred_element_type=F32)
            res = res + ag1[:, c, :, cols].astype(F32).reshape(qc, tile)
            aft[:, :, cols] = res.astype(BF16).reshape(T, cr, tile)

        loop(width // tile, cols_of)
        normed[...] = rms_norm(aft[...].astype(F32).reshape(qc, width), mlp_gain[...])
        own[c] = aft[z].astype(F32)

    def feed_up():
        def cols_of(n):
            cols = pl.ds(pl.multiple_of(n * tile, tile), tile)
            res = jnp.dot(normed[...], w_up[:, cols], preferred_element_type=F32)
            upbuf[:, cols] = jax.nn.gelu(res, approximate=True).astype(BF16)

        loop(ff // tile, cols_of)

    def feed_down(c):
        def cols_of(n):
            cols = pl.ds(pl.multiple_of(n * tile, tile), tile)
            res = jnp.dot(upbuf[...], w_down[:, cols], preferred_element_type=F32)
            part[c, :, :, cols] = res.astype(BF16).reshape(T, cr, tile)

        loop(width // tile, cols_of)

    for n in range(T * NH - LAG, T * NH):
        kv_relay(jnp.int32(n))
    w_step(1)
    loop(T * NH, kv_rest)
    w_step(2)

    def when(cond, *steps):
        @pl.when(cond)
        def _():
            for step, *args in steps:
                step(*args)

    def mix(t):
        attend(t)
        when(ends | (t < 1), (mx_begin, t))
        when(t == 0, *[(w_step, k) for k in range(3, T)], (w_spread, 1))
        when(t == 1, (w_spread, 2), (w_diagonal, 1), (mx_step, 0, 1))
        when(jnp.logical_not(ends) & (t == 1), (mx_begin, 1))
        when(t == 2, *[(w_spread, k) for k in range(3, T)], (w_diagonal, 2), (mx_step, 0, 2))

    loop(C, mix)
    for k in range(3, T):
        mx_step(0, k)
        w_diagonal(k)
    for k in range(1, T):
        w_finish(k)
    loads[2].wait()
    loads[3].wait()

    near = [p for p in passes if p[0] == 1]
    far = [p for p in passes if p[0] > 1]

    def chunk(c):
        more = c + 1 < C
        project_out(c)
        when(c >= 2, *[(rs_pass, c - 2, *p) for p in far])
        when(more, (mx_step, c + 1, 1))
        when(jnp.logical_not(ends) & (c + 2 < C), (mx_begin, c + 2))
        feed_up()
        when(more, (mx_step, c + 1, 2))
        feed_down(c)
        rs_open(c)
        when(more, *[(mx_step, c + 1, k) for k in range(3, T)])
        when(c >= 1, *[(rs_pass, c - 1, *p) for p in near])

    loop(C, chunk)

    def flush(c):
        for p in far:
            rs_pass(c, *p)
        rs_finish(c)

    loop(C - 2, rs_finish)
    flush(C - 2)
    for p in near:
        rs_pass(C - 1, *p)
    flush(C - 1)

    out = hidden[...].astype(F32).reshape(rows, width)
    sums = jnp.sum(out, axis=0, keepdims=True)
    chunks = width // LANES
    for c in range(chunks):
        fsum[z, c : c + 1, :] = sums[:, c * LANES : (c + 1) * LANES]

    def fs_send(d):
        return zcopy(fsum.at[z], fsum.at[z], fs_s.at[d], fs_r.at[z], lax.rem(z + d, T))

    for d in range(1, T):
        fs_send(d).start()
    for d in range(1, T):
        o = lax.rem(z + T - d, T)
        zcopy(fsum.at[o], fsum.at[o], fs_s.at[0], fs_r.at[o], right).wait_recv()
    per = T // fr_dev
    for f in range(fr_dev):
        m = fsum[f * per]
        for s in range(f * per + 1, (f + 1) * per):
            m = m + fsum[s]
        means[roll, me, f] = m / TOK_FRAME

    def mn_send(i, peer):
        return rcopy(means.at[roll, me], means.at[roll, me], mn_s.at[i], mn_r.at[roll, me], peer)

    for i, peer in enumerate(peers):
        mn_send(i, peer).start()
    for a in range(DP):
        for b in range(S):
            if a or b:
                ra, sb = (lax.rem(roll + a, DP), lax.rem(me + b, S))
                rcopy(
                    means.at[ra, sb], means.at[ra, sb], mn_s.at[0], mn_r.at[ra, sb], peers[0]
                ).wait_recv()

    frames = S * fr_dev
    row = lax.broadcasted_iota(jnp.int32, (frames, 1), 0)
    values, gaps, valids = ([], [], [])
    for r in range(DP):
        span = lens[r]

        def frame(f, state):
            m = means[r, lax.div(f, fr_dev), lax.rem(f, fr_dev)]
            gate = jax.nn.sigmoid(m * pool_gain[...] + pool_bias[...])
            new = gate * state + (1.0 - gate) * m
            state = jnp.where(f < span, new, state)
            dots[r, pl.ds(f, 1)] = jnp.sum(state * value_weight[...], axis=0, keepdims=True)
            return state

        lax.fori_loop(0, frames, frame, jnp.zeros((chunks, LANES), F32), unroll=min(frames, 8))
        ok = row < span
        vec = jnp.where(ok, jnp.sum(dots[r], axis=1, keepdims=True), 0.0)
        reward = jnp.sum(jnp.where(row == span - 1, vec, 0.0), axis=0, keepdims=True)
        values.append(vec)
        valids.append(ok)
        gaps.append(jnp.where(ok, reward - vec, 0.0))
    count = sum(lens[r] for r in range(DP)).astype(F32)
    mean = sum(jnp.sum(g, axis=0, keepdims=True) for g in gaps) / count
    centered = [jnp.where(ok, g - mean, 0.0) for ok, g in zip(valids, gaps)]
    variance = sum(jnp.sum(c * c, axis=0, keepdims=True) for c in centered) / count
    for r in range(DP):
        small[r] = jnp.broadcast_to(values[r], (frames, LANES))
        small[DP + r] = jnp.broadcast_to(
            jnp.where(valids[r], centered[r] * lax.rsqrt(variance + 1e-05), 0.0), (frames, LANES)
        )

    for h in range(NH):

        @pl.when(z < T - 1)
        def _(h=h):
            own_send(h, 0).wait_send()

        @pl.when(z > 0)
        def _(h=h):
            own_send(h, 1).wait_send()

    for k in range(1, T):
        for s, here, way, more in sides(k):

            @pl.when(here & more)
            def _(s=s, way=way):
                for h in range(NH):
                    tok_send(s, h, way).wait_send()

                def sent(c):
                    mx_send(c, s, way).wait_send()

                loop(C, sent)

        w_drain(k)
    for way, more in ((0, z < T - 1), (1, z > 0)):

        @pl.when(more)
        def _(way=way):
            for f in range(2):
                wz_send(z, f, way).wait_send()

            def sent(c):
                mx_send(c, z, way).wait_send()

            loop(C, sent)

    def rs_drain(c):
        for d in range(T):

            @pl.when(z < d)
            def _(d=d):
                rs_send(c, d, 0, False).wait_send()

            @pl.when(z > d)
            def _(d=d):
                rs_send(c, d, 1, False).wait_send()

    loop(C, rs_drain)

    def kv_drain(n):
        s, h = (lax.div(n, NH), lax.rem(n, NH))
        for i in range(2):
            for d in range(1, S):

                @pl.when(kv_direct(d))
                def _(d=d, i=i):
                    kv_send(d, s, h, i).wait_send()

            if square:

                @pl.when(relays(i))
                def _(i=i):
                    kv_relay_copy(s, h, i).wait_send()

    loop(T * NH, kv_drain)
    for d in range(1, T):
        fs_send(d).wait_send()
    for i, peer in enumerate(peers):
        mn_send(i, peer).wait_send()


def local(
    tokens, attn_gain, w_qkv, w_out, mlp_gain, w_up, w_down, pool_gain, pool_bias, value_weight,
    valid_frames,
):
    T, S, DP = (lax.axis_size("tensor"), lax.axis_size("seq"), lax.axis_size("dp"))
    rows, width = tokens.shape[1:]
    block = rows * T
    fr_dev = block // TOK_FRAME
    chunks = width // LANES
    hcols = w_qkv.shape[2]
    heads = hcols // HEAD_DIM
    C, NH = (CHUNKS, HALVES)
    cr = rows // C
    qc = T * cr
    NP = DP * S
    assert TOK_FRAME % rows == 0 and S * fr_dev <= LANES and DP == 2
    vm = pl.BlockSpec(memory_space=pltpu.VMEM)
    hbm = pl.BlockSpec(memory_space=pl.ANY)
    dma = pltpu.SemaphoreType.DMA
    frames = S * fr_dev
    hidden, small = pl.pallas_call(
        kernel,
        out_shape=(
            jax.ShapeDtypeStruct((C, cr, width), BF16),
            jax.ShapeDtypeStruct((2 * DP, frames, LANES), F32),
        ),
        in_specs=[vm, vm, hbm, hbm, vm, hbm, hbm, vm, vm, vm, pl.BlockSpec(memory_space=pltpu.SMEM)],
        out_specs=(vm, vm),
        scratch_shapes=[
            pltpu.VMEM(w_qkv.shape, BF16),
            pltpu.VMEM((T, NP, hcols // NP, width), BF16),
            pltpu.VMEM(w_up.shape, BF16),
            pltpu.VMEM(w_down.shape, BF16),
            pltpu.VMEM((T, C, cr, width), BF16),
            pltpu.VMEM((T, C, cr, hcols), BF16),
            pltpu.VMEM((S, T, NH, 2, rows // NH, hcols), BF16),
            pltpu.VMEM((heads, 1, qc), F32),
            pltpu.VMEM((heads, 1, qc), F32),
            pltpu.VMEM((heads, HEAD_DIM, qc), F32),
            pltpu.VMEM((C, T, qc, hcols), BF16),
            pltpu.VMEM((T, cr, width), BF16),
            pltpu.VMEM((C, cr, width), F32),
            pltpu.VMEM((qc, width), BF16),
            pltpu.VMEM((qc, w_up.shape[1]), BF16),
            pltpu.VMEM((C, T, cr, width), BF16),
            pltpu.VMEM((C, 2, T, cr, width), BF16),
            pltpu.VMEM((T, chunks, LANES), F32),
            pltpu.VMEM((DP, S, fr_dev, chunks, LANES), F32),
            pltpu.VMEM((DP, frames, LANES), F32),
            dma((4,)),
            dma((2, T, NH)),
            dma((T, NH)),
            dma((S, T, NH, 2)),
            dma((S, T, NH, 2)),
            dma((T, NH, 2)),
            dma((2, T, 2)),
            dma((S, T, 2)),
            dma((T, 2)),
            dma((S, T, 2)),
            dma((T, NP, 2)),
            dma((2, C, T)),
            dma((C, T)),
            dma((2, C, T)),
            dma((2, C, T)),
            dma((T,)),
            dma((T,)),
            dma((DP * S,)),
            dma((DP, S)),
        ],
        compiler_params=pltpu.CompilerParams(
            collective_id=0, has_side_effects=True, vmem_limit_bytes=67043328
        ),
    )(
        tokens.reshape(C, cr, width),
        attn_gain[None],
        w_qkv,
        w_out.reshape(NP, hcols // NP, width),
        mlp_gain[None],
        w_up,
        w_down,
        pool_gain.reshape(chunks, LANES),
        pool_bias.reshape(chunks, LANES),
        value_weight.reshape(chunks, LANES),
        valid_frames,
    )
    roll, seq = (lax.axis_index("dp"), lax.axis_index("seq"))
    values = lax.dynamic_slice(small, (roll, seq * fr_dev, 0), (1, fr_dev, 1))[..., 0]
    advantages = lax.dynamic_slice(small, (DP + roll, seq * fr_dev, 0), (1, fr_dev, 1))[..., 0]
    return (hidden.reshape(1, rows, width), values, advantages)


def solution(mesh):
    in_specs = (
        P("dp", ("seq", "tensor"), None),
        P(),
        P(None, None, "tensor"),
        P("tensor", None),
        P(),
        P(None, "tensor"),
        P("tensor", None),
        P(),
        P(),
        P(),
        P(),
    )
    out_specs = (P("dp", ("seq", "tensor"), None), P("dp", "seq"), P("dp", "seq"))
    return jax.shard_map(local, mesh=mesh, in_specs=in_specs, out_specs=out_specs, check_vma=False)
```

```python
import math

import jax
import jax.numpy as jnp
from jax import lax
from jax.experimental import pallas as pl
from jax.experimental.pallas import tpu as pltpu
from jax.sharding import PartitionSpec as P

HEAD_DIM = 128
TOK_FRAME = 256
LANES = 128
CHUNKS = 4
HALVES = 2
PIECES = 2
GROUP = 4
EARLY = 4
MESH = pl.DeviceIdType.MESH
F32 = jnp.float32
BF16 = jnp.bfloat16


def rms_norm(floats, gain):
    square = jnp.mean(floats * floats, axis=-1, keepdims=True)
    return (floats * lax.rsqrt(square + 1e-05) * gain).astype(BF16)


def loop(n, body):
    def step(i, carry):
        body(i)
        return carry

    lax.fori_loop(0, n, step, 0)


def kernel(
    tok, attn_gain, w_qkv_h, w_out_h, mlp_gain, w_up_h, w_down_h, pool_gain, pool_bias,
    value_weight, lens,
    hidden, small,
    w_qkv, w_out, w_up, w_down, ag1, query, kv, peak, total, acc, mixed, aft, own, normed,
    upbuf, part, rs, fsum, means, dots,
    wsem, ag_s, ag_r, kv_s, kv_r, kvr_s, wz_s, wp_s, wr_s, wd_s, wo_r, wo_p, mx_s, mx_r, rs_s, rs_r,
    fs_s, fs_r, mn_s, mn_r,
):
    T, S, DP = (lax.axis_size("tensor"), lax.axis_size("seq"), lax.axis_size("dp"))
    z, me, roll = (lax.axis_index("tensor"), lax.axis_index("seq"), lax.axis_index("dp"))
    C, cr, width = tok.shape
    rows = C * cr
    block = rows * T
    qc = T * cr
    NH = HALVES
    per_half = C // NH
    hr = rows // NH
    hcols = query.shape[-1]
    heads = hcols // HEAD_DIM
    ff = w_up.shape[1]
    fr_dev = block // TOK_FRAME
    square = S == 4
    right, left = (lax.rem(z + 1, T), lax.rem(z + T - 1, T))
    tile = 1024
    ends = (z == 0) | (z == T - 1)
    mine = roll * S + me
    other = lax.rem(roll + 1, DP)

    loads = [
        pltpu.make_async_copy(src, dst, wsem.at[i])
        for i, (src, dst) in enumerate(
            ((w_qkv_h, w_qkv), (w_out_h, w_out.at[z]), (w_up_h, w_up), (w_down_h, w_down))
        )
    ]
    for load in loads:
        load.start()

    barrier = pltpu.get_barrier_semaphore()
    for d in range(1, T):
        pl.semaphore_signal(barrier, 1, device_id={"tensor": lax.rem(z + d, T)}, device_id_type=MESH)
    peers = []
    for a in range(DP):
        for b in range(S):
            if a or b:
                peers.append({"dp": lax.rem(roll + a, DP), "seq": lax.rem(me + b, S)})
    for peer in peers:
        pl.semaphore_signal(barrier, 1, device_id=peer, device_id_type=MESH)
    pl.semaphore_wait(barrier, T - 1 + len(peers))

    def rcopy(src, dst, s_sem, r_sem, to):
        return pltpu.make_async_remote_copy(
            src_ref=src, dst_ref=dst, send_sem=s_sem, recv_sem=r_sem, device_id=to,
            device_id_type=MESH,
        )

    def zcopy(src, dst, s_sem, r_sem, to):
        return rcopy(src, dst, s_sem, r_sem, {"tensor": to})

    def toward(way):
        return right if way == 0 else left

    def tok_send(s, h, way, src=None):
        ref = ag1.at[s, pl.ds(h * per_half, per_half)]
        return zcopy(ref if src is None else src, ref, ag_s.at[way, s], ag_r.at[s, h], toward(way))

    def own_send(h, way):
        return tok_send(z, h, way, tok.at[pl.ds(h * per_half, per_half)])

    for h in range(NH):

        @pl.when(z < T - 1)
        def _(h=h):
            own_send(h, 0).start()

        @pl.when(z > 0)
        def _(h=h):
            own_send(h, 1).start()

    def arrival(u):
        near = jnp.minimum(z, T - 1 - z)
        paired = u <= 2 * near
        k = jnp.where(paired, lax.div(u + 1, 2), u - near)
        odd = lax.rem(u, 2)
        longer = jnp.where(z > T - 1 - z, 1, 0)
        from_left = jnp.where(paired, odd, longer)
        return (jnp.where(from_left == 1, z - k, z + k), from_left)

    def kv_copy(j, s, h, i, sem, to):
        ref = kv.at[j, s, h, i]
        return rcopy(ref, ref, sem, kv_r.at[j, s, h, i], {"seq": to})

    def kv_send(d, s, h, i):
        return kv_copy(me, s, h, i, kv_s.at[d], lax.rem(me + d, S))

    def kv_direct(d):
        cond = me + d < S
        if square and d == 3:
            cond = cond & (me != 0)
        if square and d == 1:
            cond = cond & (me != 1)
        return cond

    relay_from = jnp.where(me == 3, 1, 0)
    relay_to = jnp.where(me == 3, 2, 3)

    def relays(i):
        return (me == 3) | (me == 1 + i)

    def kv_relay_copy(s, h, i):
        return kv_copy(relay_from, s, h, i, kvr_s.at[0], relay_to)

    def kv_relay(n):
        if square:
            s, _ = arrival(lax.div(n, NH))
            h = lax.rem(n, NH)
            for i in range(2):

                @pl.when(relays(i))
                def _(i=i):
                    copy = kv_relay_copy(s, h, i)
                    copy.wait_recv()
                    copy.start()

    def kv_rest(n):
        s, h = (lax.div(n, NH), lax.rem(n, NH))

        def source(j, carry):
            for i in range(2):
                cond = j < me
                if square:
                    cond = cond & jnp.logical_not(relays(i) & (j == relay_from))

                @pl.when(cond)
                def _(i=i):
                    kv_copy(j, s, h, i, kv_s.at[0], lax.rem(me + 1, S)).wait_recv()

            return carry

        lax.fori_loop(0, S - 1, source, 0)

    def project(s, h):
        floats = ag1[s, pl.ds(h * per_half, per_half)].astype(F32).reshape(hr, width)
        x = rms_norm(floats, attn_gain[...])
        for i in range(2):
            kv[me, s, h, i] = jnp.dot(x, w_qkv[1 + i], preferred_element_type=F32).astype(BF16)
            for d in range(1, S):

                @pl.when(kv_direct(d))
                def _(d=d, i=i):
                    kv_send(d, s, h, i).start()

        q = jnp.dot(x, w_qkv[0], preferred_element_type=F32).astype(BF16)
        query[s, pl.ds(h * per_half, per_half)] = q.reshape(per_half, cr, hcols)

    def w_ref(zz, r, f):
        half = w_out.shape[2] // 2
        return w_out.at[zz, r, pl.ds(f * half, half)]

    def w_copy(zz, b, f, sem, to):
        ref = w_ref(zz, roll * S + b, f)
        return rcopy(ref, ref, sem, wo_r.at[zz, b, f], to)

    def wz_send(zz, f, way):
        return w_copy(zz, me, f, wz_s.at[way, zz], {"tensor": toward(way)})

    flip_x = me + 1 - 2 * lax.rem(me, 2)
    flip_y = lax.rem(me + 2, 4)
    flip_d = flip_x + 2 - 4 * lax.div(flip_x, 2)

    def plane_targets():
        if square:
            return [flip_x, flip_y]
        return [lax.rem(me + d, S) for d in range(1, S)]

    def plane_sends(zz, f):
        return [
            w_copy(zz, me, f, wp_s.at[n], {"seq": to})
            for n, to in enumerate(plane_targets())
        ]

    def die_send(zz, b, f):
        ref = w_ref(zz, roll * S + b, f)
        return rcopy(ref, ref, wd_s.at[0], wo_p.at[0], {"dp": other})

    def w_arrive(zz, b, f):
        w_copy(zz, b, f, wz_s.at[0, 0], {"dp": other}).wait_recv()

    def w_relay(zz, axis):
        if axis == 0:
            return w_copy(zz, flip_x, 0, wr_s.at[0], {"seq": flip_y})
        return w_copy(zz, flip_y, 1, wr_s.at[1], {"seq": flip_x})

    def w_begin(early):
        outward = 2 * z >= T
        for f in range(2):

            @pl.when((z < T - 1) & ((ends | outward) == early))
            def _(f=f):
                wz_send(z, f, 0).start()

            @pl.when((z > 0) & ((ends | jnp.logical_not(outward)) == early))
            def _(f=f):
                wz_send(z, f, 1).start()

    def sides(k):
        return ((z - k, z - k >= 0, 0, z < T - 1), (z + k, z + k < T, 1, z > 0))

    def w_step(k):
        for zz, here, way, more in sides(k):

            @pl.when(here)
            def _(zz=zz, way=way, more=more):
                for f in range(2):
                    wz_send(zz, f, way).wait_recv()

                    @pl.when(more)
                    def _(f=f):
                        wz_send(zz, f, way).start()

                    for copy in plane_sends(zz, f):
                        copy.start()
                    die_send(zz, me, f).start()

    def w_spread(k):
        for zz, here, _, _ in sides(k):

            @pl.when(here)
            def _(zz=zz):
                if square:
                    for axis, b in ((0, flip_x), (1, flip_y)):
                        for f in range(2):
                            w_arrive(zz, b, f)
                        w_relay(zz, axis).start()
                        for f in range(2):
                            die_send(zz, b, f).start()
                else:
                    for d in range(1, S):
                        b = lax.rem(me + d, S)
                        for f in range(2):
                            w_arrive(zz, b, f)
                            die_send(zz, b, f).start()

    def w_diagonal(k):
        if square:
            for zz, here, _, _ in sides(k):

                @pl.when(here)
                def _(zz=zz):
                    for f in range(2):
                        w_arrive(zz, flip_d, f)
                        die_send(zz, flip_d, f).start()

    def w_bulk(sem_s, sem_r, ref):
        return rcopy(ref, ref, sem_s, sem_r, {"dp": other})

    def w_finish():
        ref = w_out.at[pl.ds(0, T - 1), pl.ds(0, S)]
        w_bulk(wd_s.at[0], wo_p.at[0], ref).wait_recv()

    def w_drain():
        first = pl.ds(0, T - 1)
        half = w_out.shape[2] // 2
        w_bulk(wd_s.at[0], wo_p.at[0], w_out.at[first, pl.ds(0, S)]).wait_send()
        for n, _ in enumerate(plane_targets()):
            w_bulk(wp_s.at[n], wo_p.at[0], w_out.at[first, 0]).wait_send()
        if square:
            for axis in range(2):
                w_bulk(wr_s.at[axis], wo_p.at[0], w_out.at[first, 0, pl.ds(0, half)]).wait_send()
        for way, more in ((0, z < T - 1), (1, z > 0)):
            for s in range(T):

                @pl.when(more & ((s <= z) if way == 0 else (s >= z)))
                def _(s=s, way=way):
                    ref = w_out.at[s, mine]
                    w_bulk(wz_s.at[way, s], wo_p.at[0], ref).wait_send()
                    ref = ag1.at[s]
                    zcopy(ref, ref, ag_s.at[way, s], ag_r.at[0, 0], toward(way)).wait_send()
                    ref = mixed.at[:, s]
                    zcopy(ref, ref, mx_s.at[way, s], mx_r.at[0, 0], toward(way)).wait_send()

                @pl.when((z < s) if way == 0 else (z > s))
                def _(s=s, way=way):
                    ref = rs.at[:, way, s]
                    zcopy(ref, ref, rs_s.at[way, s], rs_r.at[0, 0, 0, 0], toward(way)).wait_send()

        for d in range(1, S):

            @pl.when(kv_direct(d))
            def _(d=d):
                w_bulk(kv_s.at[d], wo_p.at[0], kv.at[0]).wait_send()

        if square:

            @pl.when(me == 3)
            def _():
                w_bulk(kvr_s.at[0], wo_p.at[0], kv.at[0]).wait_send()

            @pl.when((me == 1) | (me == 2))
            def _():
                w_bulk(kvr_s.at[0], wo_p.at[0], kv.at[0, :, :, 0]).wait_send()

    ag1[z] = tok[...]
    loads[0].wait()

    def gather(i):
        u, h = (lax.div(i, NH), lax.rem(i, NH))
        s, from_left = arrival(u)

        @pl.when(u > 0)
        def _():
            tok_send(s, h, 0).wait_recv()

            @pl.when((from_left == 1) & (z < T - 1))
            def _():
                tok_send(s, h, 0).start()

            @pl.when((from_left == 0) & (z > 0))
            def _():
                tok_send(s, h, 1).start()

        @pl.when(i == NH)
        def _():
            loads[1].wait()
            w_begin(True)

        lag = jnp.where(ends, 1, 2)

        @pl.when(i >= lag)
        def _():
            kv_relay(i - lag)

        project(s, h)

        @pl.when(ends & (i == EARLY))
        def _():
            w_step(1)


    loop(T * NH, gather)

    w_begin(False)

    length = lens[roll]
    to_bits = math.log2(math.e) / HEAD_DIM**0.5

    def attend(c):
        peak[...] = jnp.full_like(peak, -1e30)
        total[...] = jnp.zeros_like(total)
        acc[...] = jnp.zeros_like(acc)
        q_row = lax.div(lax.broadcasted_iota(jnp.int32, (fr_dev, 1, qc), 2), cr) * rows
        q_frame = me * fr_dev + lax.div(q_row, TOK_FRAME)
        k_local = lax.broadcasted_iota(jnp.int32, (fr_dev, 1, qc), 0)

        def against(first, count):
            biases = []
            for j in range(count):
                k_frame = (first + j) * fr_dev + k_local
                biases.append(jnp.where((k_frame <= q_frame) & (k_frame < length), 0.0, -1e30))
            for h in range(heads):
                cols = slice(h * HEAD_DIM, (h + 1) * HEAD_DIM)
                q = query[:, c, :, cols].reshape(qc, HEAD_DIM)
                old, norm, out = (peak[h], total[h], acc[h])
                for j in range(count):
                    k = kv[first + j, :, :, 0, :, cols].reshape(block, HEAD_DIM)
                    v = kv[first + j, :, :, 1, :, cols].reshape(block, HEAD_DIM)
                    s = lax.dot_general(k, q, (((1,), (1,)), ((), ())), preferred_element_type=F32)
                    s = s.reshape(fr_dev, TOK_FRAME, qc) * to_bits + biases[j]
                    s = s.reshape(block, qc)
                    new = jnp.maximum(old, jnp.max(s, axis=0, keepdims=True))
                    weights = jnp.exp2(s - new)
                    shrink = jnp.exp2(old - new)
                    old = new
                    norm = norm * shrink + jnp.sum(weights, axis=0, keepdims=True)
                    out = out * shrink + lax.dot_general(
                        v, weights.astype(BF16), (((0,), (0,)), ((), ())), preferred_element_type=F32
                    )
                peak[h], total[h], acc[h] = (old, norm, out)

        loop(lax.div(me + 1, GROUP), lambda g: against(g * GROUP, GROUP))
        for count in range(1, GROUP):

            @pl.when(lax.rem(me + 1, GROUP) == count)
            def _(count=count):
                against(me + 1 - count, count)

        for h in range(heads):
            cols = slice(h * HEAD_DIM, (h + 1) * HEAD_DIM)
            mixed[c, z, :, cols] = jnp.transpose(acc[h] / total[h]).astype(BF16)

    def mx_send(c, s, way):
        ref = mixed.at[c, s]
        return zcopy(ref, ref, mx_s.at[way, s], mx_r.at[c, s], toward(way))

    def mx_begin(c):
        @pl.when(z < T - 1)
        def _():
            mx_send(c, z, 0).start()

        @pl.when(z > 0)
        def _():
            mx_send(c, z, 1).start()

    def mx_step(c, k, late):
        for s, here, way, more in sides(k):

            @pl.when(here & (((s == 0) | (s == T - 1)) == late))
            def _(s=s, way=way, more=more):
                copy = mx_send(c, s, way)
                copy.wait_recv()

                @pl.when(more)
                def _():
                    copy.start()

    def rs_send(c, d, way, e, opens=False):
        span = pl.ds(e * (cr // PIECES), cr // PIECES)
        dst = rs.at[c, way, d, span]
        src = part.at[c, d, span] if opens else dst
        return zcopy(src, dst, rs_s.at[way, d], rs_r.at[way, c, d, e], toward(way))

    def rs_open(c):
        for i in range(T - 1):

            @pl.when((z == 0) & (T - 1 - i > z))
            def _(i=i):
                for e in range(PIECES):
                    rs_send(c, T - 1 - i, 0, e, True).start()

            @pl.when((z == T - 1) & (i < z))
            def _(i=i):
                for e in range(PIECES):
                    rs_send(c, i, 1, e, True).start()

    def rs_pass(c, w, i):
        for d, way, here in (
            (T - 1 - i, 0, (z == w) & (T - 1 - i > z)),
            (i, 1, (T - 1 - z == w) & (i < z)),
        ):

            @pl.when(here)
            def _(d=d, way=way):
                for e in range(PIECES):
                    span = pl.ds(e * (cr // PIECES), cr // PIECES)
                    copy = rs_send(c, d, way, e)
                    copy.wait_recv()
                    rs[c, way, d, span] = (
                        rs[c, way, d, span].astype(F32) + part[c, d, span].astype(F32)
                    ).astype(BF16)
                    copy.start()

    def rs_finish(c):
        own[c] = own[c] + part[c, z].astype(F32)

        @pl.when(z > 0)
        def _():
            for e in range(PIECES):
                rs_send(c, z, 0, e).wait_recv()
            own[c] = own[c] + rs[c, 0, z].astype(F32)

        @pl.when(z < T - 1)
        def _():
            for e in range(PIECES):
                rs_send(c, z, 1, e).wait_recv()
            own[c] = own[c] + rs[c, 1, z].astype(F32)

        hidden[c] = own[c].astype(BF16)

    passes = [(w, i) for w in range(1, T - 1) for i in range(T - 1 - w)]

    def project_out(c):
        lhs = jnp.concatenate([mixed[c, s] for s in range(T)], axis=1)

        def cols_of(n):
            cols = pl.ds(pl.multiple_of(n * tile, tile), tile)
            w = w_out[:, :, :, cols].reshape(T * hcols, tile)
            res = jnp.dot(lhs, w, preferred_element_type=F32)
            res = res + ag1[:, c, :, cols].astype(F32).reshape(qc, tile)
            aft[:, :, cols] = res.astype(BF16).reshape(T, cr, tile)

        loop(width // tile, cols_of)
        normed[...] = rms_norm(aft[...].astype(F32).reshape(qc, width), mlp_gain[...])
        own[c] = aft[z].astype(F32)

    def feed_up():
        def cols_of(n):
            cols = pl.ds(pl.multiple_of(n * tile, tile), tile)
            res = jnp.dot(normed[...], w_up[:, cols], preferred_element_type=F32)
            upbuf[:, cols] = jax.nn.gelu(res, approximate=True).astype(BF16)

        loop(ff // tile, cols_of)

    def feed_down(c):
        def cols_of(n):
            cols = pl.ds(pl.multiple_of(n * tile, tile), tile)
            res = jnp.dot(upbuf[...], w_down[:, cols], preferred_element_type=F32)
            part[c, :, :, cols] = res.astype(BF16).reshape(T, cr, tile)

        loop(width // tile, cols_of)

    @pl.when(jnp.logical_not(ends))
    def _():
        kv_relay(jnp.int32(T * NH - 2))

    kv_relay(jnp.int32(T * NH - 1))

    @pl.when(jnp.logical_not(ends))
    def _():
        w_step(1)

    w_step(2)
    loop(T * NH, kv_rest)

    def when(cond, *steps):
        @pl.when(cond)
        def _():
            for step, *args in steps:
                step(*args)

    def mix(t):
        attend(t)
        when(ends | (t == 0) | (t == C - 1), (mx_begin, t))
        when(
            t == 1,
            *[(w_step, k) for k in range(3, T)],
            (w_spread, 1),
            (mx_step, 0, 1, False),
        )
        when(t == 2, (w_spread, 2), (mx_step, 0, 2, False), (mx_step, 0, 1, True))
        when(jnp.logical_not(ends) & (t > 0) & (t < C - 1), (mx_begin, t))
        when(t == 2, (w_diagonal, 1), (mx_step, 0, 2, True))

    loop(C, mix)
    for k in range(3, T):
        w_spread(k)
    w_diagonal(2)
    for k in range(3, T):
        mx_step(0, k, False)
        mx_step(0, k, True)
        w_diagonal(k)
    mx_step(1, 1, False)
    w_finish()
    loads[2].wait()
    loads[3].wait()

    near = [p for p in passes if p[0] == 1]
    far = [p for p in passes if p[0] > 1]

    def chunk(c):
        after, later = (c + 1 < C, c + 2 < C)
        project_out(c)
        when(c >= 2, *[(rs_pass, c - 2, *p) for p in far])
        feed_up()
        when(c == 0, (mx_step, 1, 1, True), (mx_step, 1, 2, False))
        feed_down(c)
        rs_open(c)
        when(after, (mx_step, c + 1, 2, True))
        when(later, (mx_step, c + 2, 1, False), (mx_step, c + 2, 1, True), (mx_step, c + 2, 2, False))
        when(c >= 1, *[(rs_pass, c - 1, *p) for p in near])
        for k in range(3, T):
            when(after, (mx_step, c + 1, k, False), (mx_step, c + 1, k, True))

    loop(C, chunk)

    def flush(c):
        for p in far:
            rs_pass(c, *p)
        rs_finish(c)

    loop(C - 2, rs_finish)
    flush(C - 2)
    for p in near:
        rs_pass(C - 1, *p)
    flush(C - 1)

    out = hidden[...].astype(F32).reshape(rows, width)
    sums = jnp.sum(out, axis=0, keepdims=True)
    chunks = width // LANES
    for c in range(chunks):
        fsum[z, c : c + 1, :] = sums[:, c * LANES : (c + 1) * LANES]

    def fs_send(d):
        return zcopy(fsum.at[z], fsum.at[z], fs_s.at[d], fs_r.at[z], lax.rem(z + d, T))

    for d in range(1, T):
        fs_send(d).start()
    for d in range(1, T):
        o = lax.rem(z + T - d, T)
        zcopy(fsum.at[o], fsum.at[o], fs_s.at[0], fs_r.at[o], right).wait_recv()
    per = T // fr_dev
    for f in range(fr_dev):
        m = fsum[f * per]
        for s in range(f * per + 1, (f + 1) * per):
            m = m + fsum[s]
        means[roll, me, f] = m / TOK_FRAME

    def mn_send(i, peer):
        return rcopy(means.at[roll, me], means.at[roll, me], mn_s.at[i], mn_r.at[roll, me], peer)

    for i, peer in enumerate(peers):
        mn_send(i, peer).start()
    for a in range(DP):
        for b in range(S):
            if a or b:
                ra, sb = (lax.rem(roll + a, DP), lax.rem(me + b, S))
                rcopy(
                    means.at[ra, sb], means.at[ra, sb], mn_s.at[0], mn_r.at[ra, sb], peers[0]
                ).wait_recv()

    frames = S * fr_dev
    row = lax.broadcasted_iota(jnp.int32, (frames, 1), 0)
    values, gaps, valids = ([], [], [])
    for r in range(DP):
        span = lens[r]

        def frame(f, state):
            m = means[r, lax.div(f, fr_dev), lax.rem(f, fr_dev)]
            gate = jax.nn.sigmoid(m * pool_gain[...] + pool_bias[...])
            new = gate * state + (1.0 - gate) * m
            state = jnp.where(f < span, new, state)
            dots[r, pl.ds(f, 1)] = jnp.sum(state * value_weight[...], axis=0, keepdims=True)
            return state

        lax.fori_loop(0, frames, frame, jnp.zeros((chunks, LANES), F32), unroll=min(frames, 8))
        ok = row < span
        vec = jnp.where(ok, jnp.sum(dots[r], axis=1, keepdims=True), 0.0)
        reward = jnp.sum(jnp.where(row == span - 1, vec, 0.0), axis=0, keepdims=True)
        values.append(vec)
        valids.append(ok)
        gaps.append(jnp.where(ok, reward - vec, 0.0))
    count = sum(lens[r] for r in range(DP)).astype(F32)
    mean = sum(jnp.sum(g, axis=0, keepdims=True) for g in gaps) / count
    centered = [jnp.where(ok, g - mean, 0.0) for ok, g in zip(valids, gaps)]
    variance = sum(jnp.sum(c * c, axis=0, keepdims=True) for c in centered) / count
    for r in range(DP):
        small[r] = jnp.broadcast_to(values[r], (frames, LANES))
        small[DP + r] = jnp.broadcast_to(
            jnp.where(valids[r], centered[r] * lax.rsqrt(variance + 1e-05), 0.0), (frames, LANES)
        )

    w_drain()
    for d in range(1, T):
        fs_send(d).wait_send()
    for i, peer in enumerate(peers):
        mn_send(i, peer).wait_send()


def local(
    tokens, attn_gain, w_qkv, w_out, mlp_gain, w_up, w_down, pool_gain, pool_bias, value_weight,
    valid_frames,
):
    T, S, DP = (lax.axis_size("tensor"), lax.axis_size("seq"), lax.axis_size("dp"))
    rows, width = tokens.shape[1:]
    block = rows * T
    fr_dev = block // TOK_FRAME
    chunks = width // LANES
    hcols = w_qkv.shape[2]
    heads = hcols // HEAD_DIM
    C, NH = (CHUNKS, HALVES)
    cr = rows // C
    qc = T * cr
    NP = DP * S
    assert TOK_FRAME % rows == 0 and S * fr_dev <= LANES and DP == 2
    vm = pl.BlockSpec(memory_space=pltpu.VMEM)
    hbm = pl.BlockSpec(memory_space=pl.ANY)
    dma = pltpu.SemaphoreType.DMA
    frames = S * fr_dev
    hidden, small = pl.pallas_call(
        kernel,
        out_shape=(
            jax.ShapeDtypeStruct((C, cr, width), BF16),
            jax.ShapeDtypeStruct((2 * DP, frames, LANES), F32),
        ),
        in_specs=[vm, vm, hbm, hbm, vm, hbm, hbm, vm, vm, vm, pl.BlockSpec(memory_space=pltpu.SMEM)],
        out_specs=(vm, vm),
        scratch_shapes=[
            pltpu.VMEM(w_qkv.shape, BF16),
            pltpu.VMEM((T, NP, hcols // NP, width), BF16),
            pltpu.VMEM(w_up.shape, BF16),
            pltpu.VMEM(w_down.shape, BF16),
            pltpu.VMEM((T, C, cr, width), BF16),
            pltpu.VMEM((T, C, cr, hcols), BF16),
            pltpu.VMEM((S, T, NH, 2, rows // NH, hcols), BF16),
            pltpu.VMEM((heads, 1, qc), F32),
            pltpu.VMEM((heads, 1, qc), F32),
            pltpu.VMEM((heads, HEAD_DIM, qc), F32),
            pltpu.VMEM((C, T, qc, hcols), BF16),
            pltpu.VMEM((T, cr, width), BF16),
            pltpu.VMEM((C, cr, width), F32),
            pltpu.VMEM((qc, width), BF16),
            pltpu.VMEM((qc, w_up.shape[1]), BF16),
            pltpu.VMEM((C, T, cr, width), BF16),
            pltpu.VMEM((C, 2, T, cr, width), BF16),
            pltpu.VMEM((T, chunks, LANES), F32),
            pltpu.VMEM((DP, S, fr_dev, chunks, LANES), F32),
            pltpu.VMEM((DP, frames, LANES), F32),
            dma((4,)),
            dma((2, T)),
            dma((T, NH)),
            dma((S,)),
            dma((S, T, NH, 2)),
            dma((1,)),
            dma((2, T)),
            dma((S,)),
            dma((2,)),
            dma((1,)),
            dma((T, S, 2)),
            dma((1,)),
            dma((2, T)),
            dma((C, T)),
            dma((2, T)),
            dma((2, C, T, PIECES)),
            dma((T,)),
            dma((T,)),
            dma((DP * S,)),
            dma((DP, S)),
        ],
        compiler_params=pltpu.CompilerParams(
            collective_id=0, has_side_effects=True, vmem_limit_bytes=67043328
        ),
    )(
        tokens.reshape(C, cr, width),
        attn_gain[None],
        w_qkv,
        w_out.reshape(NP, hcols // NP, width),
        mlp_gain[None],
        w_up,
        w_down,
        pool_gain.reshape(chunks, LANES),
        pool_bias.reshape(chunks, LANES),
        value_weight.reshape(chunks, LANES),
        valid_frames,
    )
    roll, seq = (lax.axis_index("dp"), lax.axis_index("seq"))
    values = lax.dynamic_slice(small, (roll, seq * fr_dev, 0), (1, fr_dev, 1))[..., 0]
    advantages = lax.dynamic_slice(small, (DP + roll, seq * fr_dev, 0), (1, fr_dev, 1))[..., 0]
    return (hidden.reshape(1, rows, width), values, advantages)


def solution(mesh):
    in_specs = (
        P("dp", ("seq", "tensor"), None),
        P(),
        P(None, None, "tensor"),
        P("tensor", None),
        P(),
        P(None, "tensor"),
        P("tensor", None),
        P(),
        P(),
        P(),
        P(),
    )
    out_specs = (P("dp", ("seq", "tensor"), None), P("dp", "seq"), P("dp", "seq"))
    return jax.shard_map(local, mesh=mesh, in_specs=in_specs, out_specs=out_specs, check_vma=False)
```

```python
import math

import jax
import jax.numpy as jnp
from jax import lax
from jax.experimental import pallas as pl
from jax.experimental.pallas import tpu as pltpu
from jax.sharding import PartitionSpec as P

HEAD_DIM = 128
TOK_FRAME = 256
LANES = 128
CHUNKS = 4
HALVES = 2
PIECES = 2
GROUP = 4
EARLY = 4
MESH = pl.DeviceIdType.MESH
F32 = jnp.float32
BF16 = jnp.bfloat16


def rms_norm(floats, gain):
    square = jnp.mean(floats * floats, axis=-1, keepdims=True)
    return (floats * lax.rsqrt(square + 1e-05) * gain).astype(BF16)


def loop(n, body):
    def step(i, carry):
        body(i)
        return carry

    lax.fori_loop(0, n, step, 0)


def kernel(
    tok_h, attn_gain_h, w_qkv_h, w_out_h, mlp_gain_h, w_up_h, w_down_h, pool_gain_h, pool_bias_h,
    value_weight_h, lens,
    hidden, small,
    tok, attn_gain, mlp_gain, pool_gain, pool_bias, value_weight, w_qkv, w_out, w_up, w_down, ag1, query, kv, peak, total, acc, mixed, aft, own, normed,
    upbuf, part, rs, fsum, means, dots,
    wsem, ag_s, ag_r, kv_s, kv_r, kvr_s, wz_s, wp_s, wr_s, wd_s, wo_r, wo_p, mx_s, mx_r, rs_s, rs_r,
    fs_s, fs_r, mn_s, mn_r,
):
    T, S, DP = (lax.axis_size("tensor"), lax.axis_size("seq"), lax.axis_size("dp"))
    z, me, roll = (lax.axis_index("tensor"), lax.axis_index("seq"), lax.axis_index("dp"))
    C, cr, width = tok.shape
    rows = C * cr
    block = rows * T
    qc = T * cr
    NH = HALVES
    per_half = C // NH
    hr = rows // NH
    hcols = query.shape[-1]
    heads = hcols // HEAD_DIM
    ff = w_up.shape[1]
    fr_dev = block // TOK_FRAME
    square = S == 4
    right, left = (lax.rem(z + 1, T), lax.rem(z + T - 1, T))
    tile = 1024
    ends = (z == 0) | (z == T - 1)
    mine = roll * S + me
    other = lax.rem(roll + 1, DP)

    loads = [
        pltpu.make_async_copy(src, dst, wsem.at[i])
        for i, (src, dst) in enumerate(
            (
                (tok_h, tok), (attn_gain_h, attn_gain), (w_qkv_h, w_qkv), (w_out_h, w_out.at[z]),
                (w_up_h, w_up), (w_down_h, w_down), (mlp_gain_h, mlp_gain),
                (pool_gain_h, pool_gain), (pool_bias_h, pool_bias), (value_weight_h, value_weight),
            )
        )
    ]
    for load in loads:
        load.start()

    barrier = pltpu.get_barrier_semaphore()
    for d in range(1, T):
        pl.semaphore_signal(barrier, 1, device_id={"tensor": lax.rem(z + d, T)}, device_id_type=MESH)
    peers = []
    for a in range(DP):
        for b in range(S):
            if a or b:
                peers.append({"dp": lax.rem(roll + a, DP), "seq": lax.rem(me + b, S)})
    for peer in peers:
        pl.semaphore_signal(barrier, 1, device_id=peer, device_id_type=MESH)
    loads[0].wait()
    pl.semaphore_wait(barrier, T - 1 + len(peers))

    def rcopy(src, dst, s_sem, r_sem, to):
        return pltpu.make_async_remote_copy(
            src_ref=src, dst_ref=dst, send_sem=s_sem, recv_sem=r_sem, device_id=to,
            device_id_type=MESH,
        )

    def zcopy(src, dst, s_sem, r_sem, to):
        return rcopy(src, dst, s_sem, r_sem, {"tensor": to})

    def toward(way):
        return right if way == 0 else left

    def tok_send(s, h, way, src=None):
        ref = ag1.at[s, pl.ds(h * per_half, per_half)]
        return zcopy(ref if src is None else src, ref, ag_s.at[way, s], ag_r.at[s, h], toward(way))

    def own_send(h, way):
        return tok_send(z, h, way, tok.at[pl.ds(h * per_half, per_half)])

    for h in range(NH):

        @pl.when(z < T - 1)
        def _(h=h):
            own_send(h, 0).start()

        @pl.when(z > 0)
        def _(h=h):
            own_send(h, 1).start()

    def arrival(u):
        near = jnp.minimum(z, T - 1 - z)
        paired = u <= 2 * near
        k = jnp.where(paired, lax.div(u + 1, 2), u - near)
        odd = lax.rem(u, 2)
        longer = jnp.where(z > T - 1 - z, 1, 0)
        from_left = jnp.where(paired, odd, longer)
        return (jnp.where(from_left == 1, z - k, z + k), from_left)

    def kv_copy(j, s, h, i, sem, to):
        ref = kv.at[j, s, h, i]
        return rcopy(ref, ref, sem, kv_r.at[j, s, h, i], {"seq": to})

    def kv_send(d, s, h, i):
        return kv_copy(me, s, h, i, kv_s.at[d], lax.rem(me + d, S))

    def kv_direct(d):
        cond = me + d < S
        if square and d == 3:
            cond = cond & (me != 0)
        if square and d == 1:
            cond = cond & (me != 1)
        return cond

    relay_from = jnp.where(me == 3, 1, 0)
    relay_to = jnp.where(me == 3, 2, 3)

    def relays(i):
        return (me == 3) | (me == 1 + i)

    def kv_relay_copy(s, h, i):
        return kv_copy(relay_from, s, h, i, kvr_s.at[0], relay_to)

    def kv_relay(n):
        if square:
            s, _ = arrival(lax.div(n, NH))
            h = lax.rem(n, NH)
            for i in range(2):

                @pl.when(relays(i))
                def _(i=i):
                    copy = kv_relay_copy(s, h, i)
                    copy.wait_recv()
                    copy.start()

    def kv_rest(n):
        s, h = (lax.div(n, NH), lax.rem(n, NH))

        def source(j, carry):
            for i in range(2):
                cond = j < me
                if square:
                    cond = cond & jnp.logical_not(relays(i) & (j == relay_from))

                @pl.when(cond)
                def _(i=i):
                    kv_copy(j, s, h, i, kv_s.at[0], lax.rem(me + 1, S)).wait_recv()

            return carry

        lax.fori_loop(0, S - 1, source, 0)

    def project(s, h):
        floats = ag1[s, pl.ds(h * per_half, per_half)].astype(F32).reshape(hr, width)
        x = rms_norm(floats, attn_gain[...])
        for i in range(2):
            kv[me, s, h, i] = jnp.dot(x, w_qkv[1 + i], preferred_element_type=F32).astype(BF16)
            for d in range(1, S):

                @pl.when(kv_direct(d))
                def _(d=d, i=i):
                    kv_send(d, s, h, i).start()

        q = jnp.dot(x, w_qkv[0], preferred_element_type=F32).astype(BF16)
        query[s, pl.ds(h * per_half, per_half)] = q.reshape(per_half, cr, hcols)

    def w_ref(zz, r, f):
        half = w_out.shape[2] // 2
        return w_out.at[zz, r, pl.ds(f * half, half)]

    def w_copy(zz, b, f, sem, to):
        ref = w_ref(zz, roll * S + b, f)
        return rcopy(ref, ref, sem, wo_r.at[zz, b, f], to)

    def wz_send(zz, f, way):
        return w_copy(zz, me, f, wz_s.at[way, zz], {"tensor": toward(way)})

    flip_x = me + 1 - 2 * lax.rem(me, 2)
    flip_y = lax.rem(me + 2, 4)
    flip_d = flip_x + 2 - 4 * lax.div(flip_x, 2)

    def plane_targets():
        if square:
            return [flip_x, flip_y]
        return [lax.rem(me + d, S) for d in range(1, S)]

    def plane_sends(zz, f):
        return [
            w_copy(zz, me, f, wp_s.at[n], {"seq": to})
            for n, to in enumerate(plane_targets())
        ]

    def die_send(zz, b, f):
        ref = w_ref(zz, roll * S + b, f)
        return rcopy(ref, ref, wd_s.at[0], wo_p.at[0], {"dp": other})

    def w_arrive(zz, b, f):
        w_copy(zz, b, f, wz_s.at[0, 0], {"dp": other}).wait_recv()

    def w_relay(zz, axis):
        if axis == 0:
            return w_copy(zz, flip_x, 0, wr_s.at[0], {"seq": flip_y})
        return w_copy(zz, flip_y, 1, wr_s.at[1], {"seq": flip_x})

    def w_begin(early):
        outward = 2 * z >= T
        for f in range(2):

            @pl.when((z < T - 1) & ((ends | outward) == early))
            def _(f=f):
                wz_send(z, f, 0).start()

            @pl.when((z > 0) & ((ends | jnp.logical_not(outward)) == early))
            def _(f=f):
                wz_send(z, f, 1).start()

    def sides(k):
        return ((z - k, z - k >= 0, 0, z < T - 1), (z + k, z + k < T, 1, z > 0))

    def w_step(k):
        for zz, here, way, more in sides(k):

            @pl.when(here)
            def _(zz=zz, way=way, more=more):
                for f in range(2):
                    wz_send(zz, f, way).wait_recv()

                    @pl.when(more)
                    def _(f=f):
                        wz_send(zz, f, way).start()

                    for copy in plane_sends(zz, f):
                        copy.start()
                    die_send(zz, me, f).start()

    def w_spread(k):
        for zz, here, _, _ in sides(k):

            @pl.when(here)
            def _(zz=zz):
                if square:
                    sources = ((0, flip_x), (1, flip_y))
                    for axis, b in sources:
                        w_arrive(zz, b, axis)
                        w_relay(zz, axis).start()
                    for axis, b in sources:
                        w_arrive(zz, b, 1 - axis)
                        for f in range(2):
                            die_send(zz, b, f).start()
                else:
                    for d in range(1, S):
                        b = lax.rem(me + d, S)
                        for f in range(2):
                            w_arrive(zz, b, f)
                            die_send(zz, b, f).start()

    def w_diagonal(k):
        if square:
            for zz, here, _, _ in sides(k):

                @pl.when(here)
                def _(zz=zz):
                    for f in range(2):
                        w_arrive(zz, flip_d, f)
                        die_send(zz, flip_d, f).start()

    def w_bulk(sem_s, sem_r, ref):
        return rcopy(ref, ref, sem_s, sem_r, {"dp": other})

    def w_finish():
        ref = w_out.at[pl.ds(0, T - 1), pl.ds(0, S)]
        w_bulk(wd_s.at[0], wo_p.at[0], ref).wait_recv()

    def w_drain():
        first = pl.ds(0, T - 1)
        half = w_out.shape[2] // 2
        w_bulk(wd_s.at[0], wo_p.at[0], w_out.at[first, pl.ds(0, S)]).wait_send()
        for n, _ in enumerate(plane_targets()):
            w_bulk(wp_s.at[n], wo_p.at[0], w_out.at[first, 0]).wait_send()
        if square:
            for axis in range(2):
                w_bulk(wr_s.at[axis], wo_p.at[0], w_out.at[first, 0, pl.ds(0, half)]).wait_send()
        for way, more in ((0, z < T - 1), (1, z > 0)):
            for s in range(T):

                @pl.when(more & ((s <= z) if way == 0 else (s >= z)))
                def _(s=s, way=way):
                    ref = w_out.at[s, mine]
                    w_bulk(wz_s.at[way, s], wo_p.at[0], ref).wait_send()
                    ref = ag1.at[s]
                    zcopy(ref, ref, ag_s.at[way, s], ag_r.at[0, 0], toward(way)).wait_send()
                    ref = mixed.at[:, s]
                    zcopy(ref, ref, mx_s.at[way, s], mx_r.at[0, 0], toward(way)).wait_send()

                @pl.when((z < s) if way == 0 else (z > s))
                def _(s=s, way=way):
                    ref = rs.at[:, way, s]
                    zcopy(ref, ref, rs_s.at[way, s], rs_r.at[0, 0, 0, 0], toward(way)).wait_send()

        for d in range(1, S):

            @pl.when(kv_direct(d))
            def _(d=d):
                w_bulk(kv_s.at[d], wo_p.at[0], kv.at[0]).wait_send()

        if square:

            @pl.when(me == 3)
            def _():
                w_bulk(kvr_s.at[0], wo_p.at[0], kv.at[0]).wait_send()

            @pl.when((me == 1) | (me == 2))
            def _():
                w_bulk(kvr_s.at[0], wo_p.at[0], kv.at[0, :, :, 0]).wait_send()

    ag1[z] = tok[...]
    loads[1].wait()
    loads[2].wait()

    def gather(i):
        u, h = (lax.div(i, NH), lax.rem(i, NH))
        s, from_left = arrival(u)

        @pl.when(u > 0)
        def _():
            tok_send(s, h, 0).wait_recv()

            @pl.when((from_left == 1) & (z < T - 1))
            def _():
                tok_send(s, h, 0).start()

            @pl.when((from_left == 0) & (z > 0))
            def _():
                tok_send(s, h, 1).start()

        @pl.when(i == NH)
        def _():
            loads[3].wait()
            w_begin(True)

        lag = jnp.where(ends, 1, 2)

        @pl.when(i >= lag)
        def _():
            kv_relay(i - lag)

        project(s, h)

        @pl.when(ends & (i == EARLY))
        def _():
            w_step(1)


    loop(T * NH, gather)

    w_begin(False)

    length = lens[roll]
    to_bits = math.log2(math.e) / HEAD_DIM**0.5

    def attend(c):
        peak[...] = jnp.full_like(peak, -1e30)
        total[...] = jnp.zeros_like(total)
        acc[...] = jnp.zeros_like(acc)
        q_row = lax.div(lax.broadcasted_iota(jnp.int32, (fr_dev, 1, qc), 2), cr) * rows
        q_frame = me * fr_dev + lax.div(q_row, TOK_FRAME)
        k_local = lax.broadcasted_iota(jnp.int32, (fr_dev, 1, qc), 0)

        def against(first, count):
            biases = []
            for j in range(count):
                k_frame = (first + j) * fr_dev + k_local
                biases.append(jnp.where((k_frame <= q_frame) & (k_frame < length), 0.0, -1e30))
            for h in range(heads):
                cols = slice(h * HEAD_DIM, (h + 1) * HEAD_DIM)
                q = query[:, c, :, cols].reshape(qc, HEAD_DIM)
                old, norm, out = (peak[h], total[h], acc[h])
                for j in range(count):
                    k = kv[first + j, :, :, 0, :, cols].reshape(block, HEAD_DIM)
                    v = kv[first + j, :, :, 1, :, cols].reshape(block, HEAD_DIM)
                    s = lax.dot_general(k, q, (((1,), (1,)), ((), ())), preferred_element_type=F32)
                    s = s.reshape(fr_dev, TOK_FRAME, qc) * to_bits + biases[j]
                    s = s.reshape(block, qc)
                    new = jnp.maximum(old, jnp.max(s, axis=0, keepdims=True))
                    weights = jnp.exp2(s - new)
                    shrink = jnp.exp2(old - new)
                    old = new
                    norm = norm * shrink + jnp.sum(weights, axis=0, keepdims=True)
                    out = out * shrink + lax.dot_general(
                        v, weights.astype(BF16), (((0,), (0,)), ((), ())), preferred_element_type=F32
                    )
                peak[h], total[h], acc[h] = (old, norm, out)

        loop(lax.div(me + 1, GROUP), lambda g: against(g * GROUP, GROUP))
        for count in range(1, GROUP):

            @pl.when(lax.rem(me + 1, GROUP) == count)
            def _(count=count):
                against(me + 1 - count, count)

        for h in range(heads):
            cols = slice(h * HEAD_DIM, (h + 1) * HEAD_DIM)
            mixed[c, z, :, cols] = jnp.transpose(acc[h] / total[h]).astype(BF16)

    def mx_send(c, s, way):
        ref = mixed.at[c, s]
        return zcopy(ref, ref, mx_s.at[way, s], mx_r.at[c, s], toward(way))

    def mx_begin(c):
        @pl.when(z < T - 1)
        def _():
            mx_send(c, z, 0).start()

        @pl.when(z > 0)
        def _():
            mx_send(c, z, 1).start()

    def mx_step(c, k, late):
        for s, here, way, more in sides(k):

            @pl.when(here & (((s == 0) | (s == T - 1)) == late))
            def _(s=s, way=way, more=more):
                copy = mx_send(c, s, way)
                copy.wait_recv()

                @pl.when(more)
                def _():
                    copy.start()

    def rs_send(c, d, way, e, opens=False):
        span = pl.ds(e * (cr // PIECES), cr // PIECES)
        dst = rs.at[c, way, d, span]
        src = part.at[c, d, span] if opens else dst
        return zcopy(src, dst, rs_s.at[way, d], rs_r.at[way, c, d, e], toward(way))

    def rs_open(c):
        for i in range(T - 1):

            @pl.when((z == 0) & (T - 1 - i > z))
            def _(i=i):
                for e in range(PIECES):
                    rs_send(c, T - 1 - i, 0, e, True).start()

            @pl.when((z == T - 1) & (i < z))
            def _(i=i):
                for e in range(PIECES):
                    rs_send(c, i, 1, e, True).start()

    def rs_pass(c, w, i):
        for d, way, here in (
            (T - 1 - i, 0, (z == w) & (T - 1 - i > z)),
            (i, 1, (T - 1 - z == w) & (i < z)),
        ):

            @pl.when(here)
            def _(d=d, way=way):
                for e in range(PIECES):
                    span = pl.ds(e * (cr // PIECES), cr // PIECES)
                    copy = rs_send(c, d, way, e)
                    copy.wait_recv()
                    rs[c, way, d, span] = (
                        rs[c, way, d, span].astype(F32) + part[c, d, span].astype(F32)
                    ).astype(BF16)
                    copy.start()

    def rs_finish(c):
        own[c] = own[c] + part[c, z].astype(F32)

        @pl.when(z > 0)
        def _():
            for e in range(PIECES):
                rs_send(c, z, 0, e).wait_recv()
            own[c] = own[c] + rs[c, 0, z].astype(F32)

        @pl.when(z < T - 1)
        def _():
            for e in range(PIECES):
                rs_send(c, z, 1, e).wait_recv()
            own[c] = own[c] + rs[c, 1, z].astype(F32)

        hidden[c] = own[c].astype(BF16)

    passes = [(w, i) for w in range(1, T - 1) for i in range(T - 1 - w)]

    def project_out(c):
        lhs = jnp.concatenate([mixed[c, s] for s in range(T)], axis=1)

        def cols_of(n):
            cols = pl.ds(pl.multiple_of(n * tile, tile), tile)
            w = w_out[:, :, :, cols].reshape(T * hcols, tile)
            res = jnp.dot(lhs, w, preferred_element_type=F32)
            res = res + ag1[:, c, :, cols].astype(F32).reshape(qc, tile)
            aft[:, :, cols] = res.astype(BF16).reshape(T, cr, tile)

        loop(width // tile, cols_of)
        normed[...] = rms_norm(aft[...].astype(F32).reshape(qc, width), mlp_gain[...])
        own[c] = aft[z].astype(F32)

    def feed_up():
        def cols_of(n):
            cols = pl.ds(pl.multiple_of(n * tile, tile), tile)
            res = jnp.dot(normed[...], w_up[:, cols], preferred_element_type=F32)
            upbuf[:, cols] = jax.nn.gelu(res, approximate=True).astype(BF16)

        loop(ff // tile, cols_of)

    def feed_down(c):
        def cols_of(n):
            cols = pl.ds(pl.multiple_of(n * tile, tile), tile)
            res = jnp.dot(upbuf[...], w_down[:, cols], preferred_element_type=F32)
            part[c, :, :, cols] = res.astype(BF16).reshape(T, cr, tile)

        loop(width // tile, cols_of)

    @pl.when(jnp.logical_not(ends))
    def _():
        kv_relay(jnp.int32(T * NH - 2))

    kv_relay(jnp.int32(T * NH - 1))

    @pl.when(jnp.logical_not(ends))
    def _():
        w_step(1)

    w_step(2)
    loop(T * NH, kv_rest)

    def when(cond, *steps):
        @pl.when(cond)
        def _():
            for step, *args in steps:
                step(*args)

    def mix(t):
        attend(t)
        when(ends | (t == 0) | (t == C - 1), (mx_begin, t))
        when(
            t == 1,
            *[(w_step, k) for k in range(3, T)],
            (w_spread, 1),
            (mx_step, 0, 1, False),
        )
        when(t == 2, (w_spread, 2), (mx_step, 0, 2, False), (mx_step, 0, 1, True))
        when(jnp.logical_not(ends) & (t > 0) & (t < C - 1), (mx_begin, t))
        when(t == 2, (w_diagonal, 1), (mx_step, 0, 2, True))

    loop(C, mix)
    for k in range(3, T):
        w_spread(k)
    w_diagonal(2)
    for k in range(3, T):
        mx_step(0, k, False)
        mx_step(0, k, True)
        w_diagonal(k)
    mx_step(1, 1, False)
    mx_step(1, 1, True)
    w_finish()
    for load in loads[4:]:
        load.wait()

    near = [p for p in passes if p[0] == 1]
    far = [p for p in passes if p[0] > 1]

    def chunk(c):
        after, later = (c + 1 < C, c + 2 < C)
        project_out(c)
        when(c == 0, (mx_step, 1, 2, False))
        feed_up()
        when(c >= 2, *[(rs_pass, c - 2, *p) for p in far])
        feed_down(c)
        rs_open(c)
        when(after, (mx_step, c + 1, 2, True))
        when(later, (mx_step, c + 2, 1, False), (mx_step, c + 2, 1, True), (mx_step, c + 2, 2, False))
        when(c >= 1, *[(rs_pass, c - 1, *p) for p in near])
        for k in range(3, T):
            when(after, (mx_step, c + 1, k, False), (mx_step, c + 1, k, True))

    loop(C, chunk)

    def flush(c):
        for p in far:
            rs_pass(c, *p)
        rs_finish(c)

    loop(C - 2, rs_finish)
    flush(C - 2)
    for p in near:
        rs_pass(C - 1, *p)
    flush(C - 1)

    out = hidden[...].astype(F32).reshape(rows, width)
    sums = jnp.sum(out, axis=0, keepdims=True)
    chunks = width // LANES
    for c in range(chunks):
        fsum[z, c : c + 1, :] = sums[:, c * LANES : (c + 1) * LANES]

    def fs_send(d):
        return zcopy(fsum.at[z], fsum.at[z], fs_s.at[d], fs_r.at[z], lax.rem(z + d, T))

    for d in range(1, T):
        fs_send(d).start()
    for d in range(1, T):
        o = lax.rem(z + T - d, T)
        zcopy(fsum.at[o], fsum.at[o], fs_s.at[0], fs_r.at[o], right).wait_recv()
    per = T // fr_dev
    for f in range(fr_dev):
        m = fsum[f * per]
        for s in range(f * per + 1, (f + 1) * per):
            m = m + fsum[s]
        means[roll, me, f] = m / TOK_FRAME

    def mn_send(i, peer):
        return rcopy(means.at[roll, me], means.at[roll, me], mn_s.at[i], mn_r.at[roll, me], peer)

    for i, peer in enumerate(peers):
        mn_send(i, peer).start()
    for a in range(DP):
        for b in range(S):
            if a or b:
                ra, sb = (lax.rem(roll + a, DP), lax.rem(me + b, S))
                rcopy(
                    means.at[ra, sb], means.at[ra, sb], mn_s.at[0], mn_r.at[ra, sb], peers[0]
                ).wait_recv()

    frames = S * fr_dev
    row = lax.broadcasted_iota(jnp.int32, (frames, 1), 0)
    values, gaps, valids = ([], [], [])
    for r in range(DP):
        span = lens[r]

        def frame(f, state):
            m = means[r, lax.div(f, fr_dev), lax.rem(f, fr_dev)]
            gate = jax.nn.sigmoid(m * pool_gain[...] + pool_bias[...])
            new = gate * state + (1.0 - gate) * m
            state = jnp.where(f < span, new, state)
            dots[r, pl.ds(f, 1)] = jnp.sum(state * value_weight[...], axis=0, keepdims=True)
            return state

        lax.fori_loop(0, frames, frame, jnp.zeros((chunks, LANES), F32), unroll=min(frames, 8))
        ok = row < span
        vec = jnp.where(ok, jnp.sum(dots[r], axis=1, keepdims=True), 0.0)
        reward = jnp.sum(jnp.where(row == span - 1, vec, 0.0), axis=0, keepdims=True)
        values.append(vec)
        valids.append(ok)
        gaps.append(jnp.where(ok, reward - vec, 0.0))
    count = sum(lens[r] for r in range(DP)).astype(F32)
    mean = sum(jnp.sum(g, axis=0, keepdims=True) for g in gaps) / count
    centered = [jnp.where(ok, g - mean, 0.0) for ok, g in zip(valids, gaps)]
    variance = sum(jnp.sum(c * c, axis=0, keepdims=True) for c in centered) / count
    for r in range(DP):
        small[r] = jnp.broadcast_to(values[r], (frames, LANES))
        small[DP + r] = jnp.broadcast_to(
            jnp.where(valids[r], centered[r] * lax.rsqrt(variance + 1e-05), 0.0), (frames, LANES)
        )

    w_drain()
    for d in range(1, T):
        fs_send(d).wait_send()
    for i, peer in enumerate(peers):
        mn_send(i, peer).wait_send()


def local(
    tokens, attn_gain, w_qkv, w_out, mlp_gain, w_up, w_down, pool_gain, pool_bias, value_weight,
    valid_frames,
):
    T, S, DP = (lax.axis_size("tensor"), lax.axis_size("seq"), lax.axis_size("dp"))
    rows, width = tokens.shape[1:]
    block = rows * T
    fr_dev = block // TOK_FRAME
    chunks = width // LANES
    hcols = w_qkv.shape[2]
    heads = hcols // HEAD_DIM
    C, NH = (CHUNKS, HALVES)
    cr = rows // C
    qc = T * cr
    NP = DP * S
    assert TOK_FRAME % rows == 0 and S * fr_dev <= LANES and DP == 2
    vm = pl.BlockSpec(memory_space=pltpu.VMEM)
    hbm = pl.BlockSpec(memory_space=pl.ANY)
    dma = pltpu.SemaphoreType.DMA
    frames = S * fr_dev
    hidden, small = pl.pallas_call(
        kernel,
        out_shape=(
            jax.ShapeDtypeStruct((C, cr, width), BF16),
            jax.ShapeDtypeStruct((2 * DP, frames, LANES), F32),
        ),
        in_specs=[hbm] * 10 + [pl.BlockSpec(memory_space=pltpu.SMEM)],
        out_specs=(vm, vm),
        scratch_shapes=[
            pltpu.VMEM((C, cr, width), BF16),
            pltpu.VMEM((1, width), F32),
            pltpu.VMEM((1, width), F32),
            pltpu.VMEM((chunks, LANES), F32),
            pltpu.VMEM((chunks, LANES), F32),
            pltpu.VMEM((chunks, LANES), F32),
            pltpu.VMEM(w_qkv.shape, BF16),
            pltpu.VMEM((T, NP, hcols // NP, width), BF16),
            pltpu.VMEM(w_up.shape, BF16),
            pltpu.VMEM(w_down.shape, BF16),
            pltpu.VMEM((T, C, cr, width), BF16),
            pltpu.VMEM((T, C, cr, hcols), BF16),
            pltpu.VMEM((S, T, NH, 2, rows // NH, hcols), BF16),
            pltpu.VMEM((heads, 1, qc), F32),
            pltpu.VMEM((heads, 1, qc), F32),
            pltpu.VMEM((heads, HEAD_DIM, qc), F32),
            pltpu.VMEM((C, T, qc, hcols), BF16),
            pltpu.VMEM((T, cr, width), BF16),
            pltpu.VMEM((C, cr, width), F32),
            pltpu.VMEM((qc, width), BF16),
            pltpu.VMEM((qc, w_up.shape[1]), BF16),
            pltpu.VMEM((C, T, cr, width), BF16),
            pltpu.VMEM((C, 2, T, cr, width), BF16),
            pltpu.VMEM((T, chunks, LANES), F32),
            pltpu.VMEM((DP, S, fr_dev, chunks, LANES), F32),
            pltpu.VMEM((DP, frames, LANES), F32),
            dma((10,)),
            dma((2, T)),
            dma((T, NH)),
            dma((S,)),
            dma((S, T, NH, 2)),
            dma((1,)),
            dma((2, T)),
            dma((S,)),
            dma((2,)),
            dma((1,)),
            dma((T, S, 2)),
            dma((1,)),
            dma((2, T)),
            dma((C, T)),
            dma((2, T)),
            dma((2, C, T, PIECES)),
            dma((T,)),
            dma((T,)),
            dma((DP * S,)),
            dma((DP, S)),
        ],
        compiler_params=pltpu.CompilerParams(
            collective_id=0, has_side_effects=True, vmem_limit_bytes=67043328
        ),
    )(
        tokens.reshape(C, cr, width),
        attn_gain[None],
        w_qkv,
        w_out.reshape(NP, hcols // NP, width),
        mlp_gain[None],
        w_up,
        w_down,
        pool_gain.reshape(chunks, LANES),
        pool_bias.reshape(chunks, LANES),
        value_weight.reshape(chunks, LANES),
        valid_frames,
    )
    roll, seq = (lax.axis_index("dp"), lax.axis_index("seq"))
    values = lax.dynamic_slice(small, (roll, seq * fr_dev, 0), (1, fr_dev, 1))[..., 0]
    advantages = lax.dynamic_slice(small, (DP + roll, seq * fr_dev, 0), (1, fr_dev, 1))[..., 0]
    return (hidden.reshape(1, rows, width), values, advantages)


def solution(mesh):
    in_specs = (
        P("dp", ("seq", "tensor"), None),
        P(),
        P(None, None, "tensor"),
        P("tensor", None),
        P(),
        P(None, "tensor"),
        P("tensor", None),
        P(),
        P(),
        P(),
        P(),
    )
    out_specs = (P("dp", ("seq", "tensor"), None), P("dp", "seq"), P("dp", "seq"))
    return jax.shard_map(local, mesh=mesh, in_specs=in_specs, out_specs=out_specs, check_vma=False)
```

```python
import math

import jax
import jax.numpy as jnp
from jax import lax
from jax.experimental import pallas as pl
from jax.experimental.pallas import tpu as pltpu
from jax.sharding import PartitionSpec as P

HEAD_DIM = 128
TOK_FRAME = 256
LANES = 128
CHUNKS = 4
HALVES = 2
PIECES = 2
GROUP = 4
EARLY = 4
MESH = pl.DeviceIdType.MESH
F32 = jnp.float32
BF16 = jnp.bfloat16


def rms_norm(floats, gain):
    square = jnp.mean(floats * floats, axis=-1, keepdims=True)
    return (floats * lax.rsqrt(square + 1e-05) * gain).astype(BF16)


def loop(n, body):
    def step(i, carry):
        body(i)
        return carry

    lax.fori_loop(0, n, step, 0)


def kernel(
    tok_h, attn_gain_h, w_qkv_h, w_out_h, mlp_gain_h, w_up_h, w_down_h, pool_gain_h, pool_bias_h,
    value_weight_h, lens,
    hidden, small,
    tok, attn_gain, mlp_gain, pool_gain, pool_bias, value_weight, w_qkv, w_out, w_up, w_down, ag1, query, kv, peak, total, acc, mixed, aft, own, normed,
    upbuf, part, rs, fsum, means, dots,
    wsem, ag_s, ag_r, kv_s, kv_r, kvr_s, wz_s, wp_s, wr_s, wd_s, wo_r, wo_p, mx_s, mx_r, rs_s, rs_r,
    fs_s, fs_r, mn_s, mn_r,
):
    T, S, DP = (lax.axis_size("tensor"), lax.axis_size("seq"), lax.axis_size("dp"))
    z, me, roll = (lax.axis_index("tensor"), lax.axis_index("seq"), lax.axis_index("dp"))
    C, cr, width = tok.shape
    rows = C * cr
    block = rows * T
    qc = T * cr
    NH = HALVES
    per_half = C // NH
    hr = rows // NH
    hcols = query.shape[-1]
    heads = hcols // HEAD_DIM
    ff = w_up.shape[1]
    fr_dev = block // TOK_FRAME
    square = S == 4
    right, left = (lax.rem(z + 1, T), lax.rem(z + T - 1, T))
    tile = 1024
    ends = (z == 0) | (z == T - 1)
    mine = roll * S + me
    other = lax.rem(roll + 1, DP)

    loads = [
        pltpu.make_async_copy(src, dst, wsem.at[i])
        for i, (src, dst) in enumerate(
            (
                (tok_h, tok), (attn_gain_h, attn_gain), (w_qkv_h, w_qkv), (w_out_h, w_out.at[z]),
                (w_up_h, w_up), (w_down_h, w_down), (mlp_gain_h, mlp_gain),
                (pool_gain_h, pool_gain), (pool_bias_h, pool_bias), (value_weight_h, value_weight),
            )
        )
    ]
    for load in loads:
        load.start()

    barrier = pltpu.get_barrier_semaphore()
    for d in range(1, T):
        pl.semaphore_signal(barrier, 1, device_id={"tensor": lax.rem(z + d, T)}, device_id_type=MESH)
    peers = []
    for a in range(DP):
        for b in range(S):
            if a or b:
                peers.append({"dp": lax.rem(roll + a, DP), "seq": lax.rem(me + b, S)})
    for peer in peers:
        pl.semaphore_signal(barrier, 1, device_id=peer, device_id_type=MESH)
    loads[0].wait()
    pl.semaphore_wait(barrier, T - 1 + len(peers))

    def rcopy(src, dst, s_sem, r_sem, to):
        return pltpu.make_async_remote_copy(
            src_ref=src, dst_ref=dst, send_sem=s_sem, recv_sem=r_sem, device_id=to,
            device_id_type=MESH,
        )

    def zcopy(src, dst, s_sem, r_sem, to):
        return rcopy(src, dst, s_sem, r_sem, {"tensor": to})

    def toward(way):
        return right if way == 0 else left

    def tok_send(s, h, way, src=None):
        ref = ag1.at[s, pl.ds(h * per_half, per_half)]
        return zcopy(ref if src is None else src, ref, ag_s.at[way, s], ag_r.at[s, h], toward(way))

    def own_send(h, way):
        return tok_send(z, h, way, tok.at[pl.ds(h * per_half, per_half)])

    for h in range(NH):

        @pl.when(z < T - 1)
        def _(h=h):
            own_send(h, 0).start()

        @pl.when(z > 0)
        def _(h=h):
            own_send(h, 1).start()

    def arrival(u):
        near = jnp.minimum(z, T - 1 - z)
        paired = u <= 2 * near
        k = jnp.where(paired, lax.div(u + 1, 2), u - near)
        odd = lax.rem(u, 2)
        longer = jnp.where(z > T - 1 - z, 1, 0)
        from_left = jnp.where(paired, odd, longer)
        return (jnp.where(from_left == 1, z - k, z + k), from_left)

    def kv_copy(j, s, h, i, sem, to, relayed):
        ref = kv.at[j, s, h, i]
        slot = jnp.where(relayed, (s * NH + h) * 2 + i, T * NH * 2 + j)
        return rcopy(ref, ref, sem, kv_r.at[slot], {"seq": to})

    def kv_send(d, s, h, i):
        relayed = me < 0
        if square and d == 1 and i == 0:
            relayed = me == 0
        if square and d == 2:
            relayed = (me == 1) | (i == 1)
        return kv_copy(me, s, h, i, kv_s.at[d], lax.rem(me + d, S), relayed)

    def kv_direct(d):
        cond = me + d < S
        if square and d == 3:
            cond = cond & (me != 0)
        if square and d == 1:
            cond = cond & (me != 1)
        return cond

    relay_from = jnp.where(me == 3, 1, 0)
    relay_to = jnp.where(me == 3, 2, 3)

    def relays(i):
        return (me == 3) | (me == 1 + i)

    def kv_relay_copy(s, h, i, arrives):
        return kv_copy(relay_from, s, h, i, kvr_s.at[0], relay_to, (me >= 0) if arrives else (me < 0))

    def kv_relay(n):
        if square:
            s, _ = arrival(lax.div(n, NH))
            h = lax.rem(n, NH)
            for i in range(2):

                @pl.when(relays(i))
                def _(i=i):
                    kv_relay_copy(s, h, i, True).wait_recv()
                    kv_relay_copy(s, h, i, False).start()

    def kv_rest(j):
        def bulk(cond, ref):
            @pl.when((j < me) & cond)
            def _():
                rcopy(ref, ref, kv_s.at[0], kv_r.at[T * NH * 2 + j], {"dp": other}).wait_recv()

        if square:
            bulk(j != relay_from, kv.at[j])
            for i in range(2):
                bulk((j == relay_from) & (me == 1 + i), kv.at[j, :, :, 1 - i])
        else:
            bulk(j >= 0, kv.at[j])

    def project(s, h):
        floats = ag1[s, pl.ds(h * per_half, per_half)].astype(F32).reshape(hr, width)
        x = rms_norm(floats, attn_gain[...])
        for i in range(2):
            kv[me, s, h, i] = jnp.dot(x, w_qkv[1 + i], preferred_element_type=F32).astype(BF16)
            for d in range(1, S):

                @pl.when(kv_direct(d))
                def _(d=d, i=i):
                    kv_send(d, s, h, i).start()

        q = jnp.dot(x, w_qkv[0], preferred_element_type=F32).astype(BF16)
        query[s, pl.ds(h * per_half, per_half)] = q.reshape(per_half, cr, hcols)

    def w_ref(zz, r, f):
        half = w_out.shape[2] // 2
        return w_out.at[zz, r, pl.ds(f * half, half)]

    def w_copy(zz, b, f, sem, to):
        ref = w_ref(zz, roll * S + b, f)
        return rcopy(ref, ref, sem, wo_r.at[zz, b, f], to)

    def wz_send(zz, f, way):
        return w_copy(zz, me, f, wz_s.at[way, zz], {"tensor": toward(way)})

    flip_x = me + 1 - 2 * lax.rem(me, 2)
    flip_y = lax.rem(me + 2, 4)
    flip_d = flip_x + 2 - 4 * lax.div(flip_x, 2)

    def plane_targets():
        if square:
            return [flip_x, flip_y]
        return [lax.rem(me + d, S) for d in range(1, S)]

    def plane_sends(zz, f):
        return [
            w_copy(zz, me, f, wp_s.at[n], {"seq": to})
            for n, to in enumerate(plane_targets())
        ]

    def die_send(zz, b, f):
        ref = w_ref(zz, roll * S + b, f)
        return rcopy(ref, ref, wd_s.at[0], wo_p.at[0], {"dp": other})

    def w_arrive(zz, b, f):
        w_copy(zz, b, f, wz_s.at[0, 0], {"dp": other}).wait_recv()

    def w_relay(zz, axis):
        if axis == 0:
            return w_copy(zz, flip_x, 0, wr_s.at[0], {"seq": flip_y})
        return w_copy(zz, flip_y, 1, wr_s.at[1], {"seq": flip_x})

    def w_begin(early):
        outward = 2 * z >= T
        for f in range(2):

            @pl.when((z < T - 1) & ((ends | outward) == early))
            def _(f=f):
                wz_send(z, f, 0).start()

            @pl.when((z > 0) & ((ends | jnp.logical_not(outward)) == early))
            def _(f=f):
                wz_send(z, f, 1).start()

    def sides(k):
        return ((z - k, z - k >= 0, 0, z < T - 1), (z + k, z + k < T, 1, z > 0))

    def w_step(k):
        for zz, here, way, more in sides(k):

            @pl.when(here)
            def _(zz=zz, way=way, more=more):
                for f in range(2):
                    wz_send(zz, f, way).wait_recv()

                    @pl.when(more)
                    def _(f=f):
                        wz_send(zz, f, way).start()

                    for copy in plane_sends(zz, f):
                        copy.start()
                    die_send(zz, me, f).start()

    def w_spread(k):
        for zz, here, _, _ in sides(k):

            @pl.when(here)
            def _(zz=zz):
                if square:
                    sources = ((0, flip_x), (1, flip_y))
                    for axis, b in sources:
                        w_arrive(zz, b, axis)
                        w_relay(zz, axis).start()
                    for axis, b in sources:
                        w_arrive(zz, b, 1 - axis)
                        for f in range(2):
                            die_send(zz, b, f).start()
                else:
                    for d in range(1, S):
                        b = lax.rem(me + d, S)
                        for f in range(2):
                            w_arrive(zz, b, f)
                            die_send(zz, b, f).start()

    def w_diagonal(k):
        if square:
            for zz, here, _, _ in sides(k):

                @pl.when(here)
                def _(zz=zz):
                    for f in range(2):
                        w_arrive(zz, flip_d, f)
                        die_send(zz, flip_d, f).start()

    def w_bulk(sem_s, sem_r, ref):
        return rcopy(ref, ref, sem_s, sem_r, {"dp": other})

    def w_finish():
        ref = w_out.at[pl.ds(0, T - 1), pl.ds(0, S)]
        w_bulk(wd_s.at[0], wo_p.at[0], ref).wait_recv()

    def w_drain():
        first = pl.ds(0, T - 1)
        half = w_out.shape[2] // 2
        w_bulk(wd_s.at[0], wo_p.at[0], w_out.at[first, pl.ds(0, S)]).wait_send()
        for n, _ in enumerate(plane_targets()):
            w_bulk(wp_s.at[n], wo_p.at[0], w_out.at[first, 0]).wait_send()
        if square:
            for axis in range(2):
                w_bulk(wr_s.at[axis], wo_p.at[0], w_out.at[first, 0, pl.ds(0, half)]).wait_send()
        for way, more in ((0, z < T - 1), (1, z > 0)):
            for s in range(T):

                @pl.when(more & ((s <= z) if way == 0 else (s >= z)))
                def _(s=s, way=way):
                    ref = w_out.at[s, mine]
                    w_bulk(wz_s.at[way, s], wo_p.at[0], ref).wait_send()
                    ref = ag1.at[s]
                    zcopy(ref, ref, ag_s.at[way, s], ag_r.at[0, 0], toward(way)).wait_send()
                    ref = mixed.at[:, s]
                    zcopy(ref, ref, mx_s.at[way, s], mx_r.at[0, 0], toward(way)).wait_send()

                @pl.when((z < s) if way == 0 else (z > s))
                def _(s=s, way=way):
                    ref = rs.at[:, way, s]
                    zcopy(ref, ref, rs_s.at[way, s], rs_r.at[0, 0, 0, 0], toward(way)).wait_send()

        for d in range(1, S):

            @pl.when(kv_direct(d))
            def _(d=d):
                w_bulk(kv_s.at[d], wo_p.at[0], kv.at[0]).wait_send()

        if square:

            @pl.when(me == 3)
            def _():
                w_bulk(kvr_s.at[0], wo_p.at[0], kv.at[0]).wait_send()

            @pl.when((me == 1) | (me == 2))
            def _():
                w_bulk(kvr_s.at[0], wo_p.at[0], kv.at[0, :, :, 0]).wait_send()

    ag1[z] = tok[...]
    loads[1].wait()
    loads[2].wait()

    def gather(i):
        u, h = (lax.div(i, NH), lax.rem(i, NH))
        s, from_left = arrival(u)

        @pl.when(u > 0)
        def _():
            tok_send(s, h, 0).wait_recv()

            @pl.when((from_left == 1) & (z < T - 1))
            def _():
                tok_send(s, h, 0).start()

            @pl.when((from_left == 0) & (z > 0))
            def _():
                tok_send(s, h, 1).start()

        @pl.when(i == NH)
        def _():
            loads[3].wait()
            w_begin(True)

        lag = jnp.where(ends, 1, 2)

        @pl.when(i >= lag)
        def _():
            kv_relay(i - lag)

        project(s, h)

        @pl.when(ends & (i == EARLY))
        def _():
            w_step(1)


    loop(T * NH, gather)

    w_begin(False)

    length = lens[roll]
    to_bits = math.log2(math.e) / HEAD_DIM**0.5

    def attend(c):
        peak[...] = jnp.full_like(peak, -1e30)
        total[...] = jnp.zeros_like(total)
        acc[...] = jnp.zeros_like(acc)
        q_row = lax.div(lax.broadcasted_iota(jnp.int32, (fr_dev, 1, qc), 2), cr) * rows
        q_frame = me * fr_dev + lax.div(q_row, TOK_FRAME)
        k_local = lax.broadcasted_iota(jnp.int32, (fr_dev, 1, qc), 0)

        def against(first, count):
            biases = []
            for j in range(count):
                k_frame = (first + j) * fr_dev + k_local
                biases.append(jnp.where((k_frame <= q_frame) & (k_frame < length), 0.0, -1e30))
            for h in range(heads):
                cols = slice(h * HEAD_DIM, (h + 1) * HEAD_DIM)
                q = query[:, c, :, cols].reshape(qc, HEAD_DIM)
                old, norm, out = (peak[h], total[h], acc[h])
                for j in range(count):
                    k = kv[first + j, :, :, 0, :, cols].reshape(block, HEAD_DIM)
                    v = kv[first + j, :, :, 1, :, cols].reshape(block, HEAD_DIM)
                    s = lax.dot_general(k, q, (((1,), (1,)), ((), ())), preferred_element_type=F32)
                    s = s.reshape(fr_dev, TOK_FRAME, qc) * to_bits + biases[j]
                    s = s.reshape(block, qc)
                    new = jnp.maximum(old, jnp.max(s, axis=0, keepdims=True))
                    weights = jnp.exp2(s - new)
                    shrink = jnp.exp2(old - new)
                    old = new
                    norm = norm * shrink + jnp.sum(weights, axis=0, keepdims=True)
                    out = out * shrink + lax.dot_general(
                        v, weights.astype(BF16), (((0,), (0,)), ((), ())), preferred_element_type=F32
                    )
                peak[h], total[h], acc[h] = (old, norm, out)

        loop(lax.div(me + 1, GROUP), lambda g: against(g * GROUP, GROUP))
        for count in range(1, GROUP):

            @pl.when(lax.rem(me + 1, GROUP) == count)
            def _(count=count):
                against(me + 1 - count, count)

        for h in range(heads):
            cols = slice(h * HEAD_DIM, (h + 1) * HEAD_DIM)
            mixed[c, z, :, cols] = jnp.transpose(acc[h] / total[h]).astype(BF16)

    def mx_send(c, s, way):
        ref = mixed.at[c, s]
        return zcopy(ref, ref, mx_s.at[way, s], mx_r.at[c, s], toward(way))

    def mx_begin(c):
        @pl.when(z < T - 1)
        def _():
            mx_send(c, z, 0).start()

        @pl.when(z > 0)
        def _():
            mx_send(c, z, 1).start()

    def mx_step(c, k, late):
        for s, here, way, more in sides(k):

            @pl.when(here & (((s == 0) | (s == T - 1)) == late))
            def _(s=s, way=way, more=more):
                copy = mx_send(c, s, way)
                copy.wait_recv()

                @pl.when(more)
                def _():
                    copy.start()

    def rs_send(c, d, way, e, opens=False):
        span = pl.ds(e * (cr // PIECES), cr // PIECES)
        dst = rs.at[c, way, d, span]
        src = part.at[c, d, span] if opens else dst
        return zcopy(src, dst, rs_s.at[way, d], rs_r.at[way, c, d, e], toward(way))

    def rs_open(c):
        for i in range(T - 1):

            @pl.when((z == 0) & (T - 1 - i > z))
            def _(i=i):
                for e in range(PIECES):
                    rs_send(c, T - 1 - i, 0, e, True).start()

            @pl.when((z == T - 1) & (i < z))
            def _(i=i):
                for e in range(PIECES):
                    rs_send(c, i, 1, e, True).start()

    def rs_pass(c, w, i):
        for d, way, here in (
            (T - 1 - i, 0, (z == w) & (T - 1 - i > z)),
            (i, 1, (T - 1 - z == w) & (i < z)),
        ):

            @pl.when(here)
            def _(d=d, way=way):
                for e in range(PIECES):
                    span = pl.ds(e * (cr // PIECES), cr // PIECES)
                    copy = rs_send(c, d, way, e)
                    copy.wait_recv()
                    rs[c, way, d, span] = (
                        rs[c, way, d, span].astype(F32) + part[c, d, span].astype(F32)
                    ).astype(BF16)
                    copy.start()

    def rs_finish(c):
        own[c] = own[c] + part[c, z].astype(F32)

        @pl.when(z > 0)
        def _():
            for e in range(PIECES):
                rs_send(c, z, 0, e).wait_recv()
            own[c] = own[c] + rs[c, 0, z].astype(F32)

        @pl.when(z < T - 1)
        def _():
            for e in range(PIECES):
                rs_send(c, z, 1, e).wait_recv()
            own[c] = own[c] + rs[c, 1, z].astype(F32)

        hidden[c] = own[c].astype(BF16)

    passes = [(w, i) for w in range(1, T - 1) for i in range(T - 1 - w)]

    def project_out(c):
        lhs = jnp.concatenate([mixed[c, s] for s in range(T)], axis=1)

        def cols_of(n):
            cols = pl.ds(pl.multiple_of(n * tile, tile), tile)
            w = w_out[:, :, :, cols].reshape(T * hcols, tile)
            res = jnp.dot(lhs, w, preferred_element_type=F32)
            res = res + ag1[:, c, :, cols].astype(F32).reshape(qc, tile)
            aft[:, :, cols] = res.astype(BF16).reshape(T, cr, tile)

        loop(width // tile, cols_of)
        normed[...] = rms_norm(aft[...].astype(F32).reshape(qc, width), mlp_gain[...])
        own[c] = aft[z].astype(F32)

    def feed_up():
        def cols_of(n):
            cols = pl.ds(pl.multiple_of(n * tile, tile), tile)
            res = jnp.dot(normed[...], w_up[:, cols], preferred_element_type=F32)
            upbuf[:, cols] = jax.nn.gelu(res, approximate=True).astype(BF16)

        loop(ff // tile, cols_of)

    def feed_down(c):
        def cols_of(n):
            cols = pl.ds(pl.multiple_of(n * tile, tile), tile)
            res = jnp.dot(upbuf[...], w_down[:, cols], preferred_element_type=F32)
            part[c, :, :, cols] = res.astype(BF16).reshape(T, cr, tile)

        loop(width // tile, cols_of)

    @pl.when(jnp.logical_not(ends))
    def _():
        kv_relay(jnp.int32(T * NH - 2))

    kv_relay(jnp.int32(T * NH - 1))

    @pl.when(jnp.logical_not(ends))
    def _():
        w_step(1)

    w_step(2)
    loop(S - 1, kv_rest)

    def when(cond, *steps):
        @pl.when(cond)
        def _():
            for step, *args in steps:
                step(*args)

    def mix(t):
        attend(t)
        when(ends | (t == 0) | (t == C - 1), (mx_begin, t))
        when(
            t == 1,
            *[(w_step, k) for k in range(3, T)],
            (w_spread, 1),
            (mx_step, 0, 1, False),
        )
        when(t == 2, (w_spread, 2), (mx_step, 0, 2, False), (mx_step, 0, 1, True))
        when(jnp.logical_not(ends) & (t > 0) & (t < C - 1), (mx_begin, t))
        when(t == 2, (w_diagonal, 1), (mx_step, 0, 2, True))

    loop(C, mix)
    for k in range(3, T):
        w_spread(k)
    w_diagonal(2)
    for k in range(3, T):
        mx_step(0, k, False)
        mx_step(0, k, True)
        w_diagonal(k)
    mx_step(1, 1, False)
    mx_step(1, 1, True)
    w_finish()
    for load in loads[4:]:
        load.wait()

    near = [p for p in passes if p[0] == 1]
    far = [p for p in passes if p[0] > 1]

    def chunk(c):
        after, later = (c + 1 < C, c + 2 < C)
        project_out(c)
        when(c == 0, (mx_step, 1, 2, False))
        feed_up()
        when(c >= 2, *[(rs_pass, c - 2, *p) for p in far])
        feed_down(c)
        rs_open(c)
        when(after, (mx_step, c + 1, 2, True))
        when(later, (mx_step, c + 2, 1, False), (mx_step, c + 2, 1, True), (mx_step, c + 2, 2, False))
        when(c >= 1, *[(rs_pass, c - 1, *p) for p in near])
        for k in range(3, T):
            when(after, (mx_step, c + 1, k, False), (mx_step, c + 1, k, True))

    loop(C, chunk)

    def flush(c):
        for p in far:
            rs_pass(c, *p)
        rs_finish(c)

    loop(C - 2, rs_finish)
    flush(C - 2)
    for p in near:
        rs_pass(C - 1, *p)
    flush(C - 1)

    out = hidden[...].astype(F32).reshape(rows, width)
    sums = jnp.sum(out, axis=0, keepdims=True)
    chunks = width // LANES
    for c in range(chunks):
        fsum[z, c : c + 1, :] = sums[:, c * LANES : (c + 1) * LANES]

    def fs_send(d):
        return zcopy(fsum.at[z], fsum.at[z], fs_s.at[d], fs_r.at[z], lax.rem(z + d, T))

    for d in range(1, T):
        fs_send(d).start()
    for d in range(1, T):
        o = lax.rem(z + T - d, T)
        zcopy(fsum.at[o], fsum.at[o], fs_s.at[0], fs_r.at[o], right).wait_recv()
    per = T // fr_dev
    for f in range(fr_dev):
        m = fsum[f * per]
        for s in range(f * per + 1, (f + 1) * per):
            m = m + fsum[s]
        means[roll, me, f] = m / TOK_FRAME

    def mn_send(i, peer):
        return rcopy(means.at[roll, me], means.at[roll, me], mn_s.at[i], mn_r.at[roll, me], peer)

    for i, peer in enumerate(peers):
        mn_send(i, peer).start()
    for a in range(DP):
        for b in range(S):
            if a or b:
                ra, sb = (lax.rem(roll + a, DP), lax.rem(me + b, S))
                rcopy(
                    means.at[ra, sb], means.at[ra, sb], mn_s.at[0], mn_r.at[ra, sb], peers[0]
                ).wait_recv()

    frames = S * fr_dev
    row = lax.broadcasted_iota(jnp.int32, (frames, 1), 0)
    values, gaps, valids = ([], [], [])
    for r in range(DP):
        span = lens[r]

        def frame(f, state):
            m = means[r, lax.div(f, fr_dev), lax.rem(f, fr_dev)]
            gate = jax.nn.sigmoid(m * pool_gain[...] + pool_bias[...])
            new = gate * state + (1.0 - gate) * m
            state = jnp.where(f < span, new, state)
            dots[r, pl.ds(f, 1)] = jnp.sum(state * value_weight[...], axis=0, keepdims=True)
            return state

        lax.fori_loop(0, frames, frame, jnp.zeros((chunks, LANES), F32), unroll=min(frames, 8))
        ok = row < span
        vec = jnp.where(ok, jnp.sum(dots[r], axis=1, keepdims=True), 0.0)
        reward = jnp.sum(jnp.where(row == span - 1, vec, 0.0), axis=0, keepdims=True)
        values.append(vec)
        valids.append(ok)
        gaps.append(jnp.where(ok, reward - vec, 0.0))
    count = sum(lens[r] for r in range(DP)).astype(F32)
    mean = sum(jnp.sum(g, axis=0, keepdims=True) for g in gaps) / count
    centered = [jnp.where(ok, g - mean, 0.0) for ok, g in zip(valids, gaps)]
    variance = sum(jnp.sum(c * c, axis=0, keepdims=True) for c in centered) / count
    for r in range(DP):
        small[r] = jnp.broadcast_to(values[r], (frames, LANES))
        small[DP + r] = jnp.broadcast_to(
            jnp.where(valids[r], centered[r] * lax.rsqrt(variance + 1e-05), 0.0), (frames, LANES)
        )

    w_drain()
    for d in range(1, T):
        fs_send(d).wait_send()
    for i, peer in enumerate(peers):
        mn_send(i, peer).wait_send()


def local(
    tokens, attn_gain, w_qkv, w_out, mlp_gain, w_up, w_down, pool_gain, pool_bias, value_weight,
    valid_frames,
):
    T, S, DP = (lax.axis_size("tensor"), lax.axis_size("seq"), lax.axis_size("dp"))
    rows, width = tokens.shape[1:]
    block = rows * T
    fr_dev = block // TOK_FRAME
    chunks = width // LANES
    hcols = w_qkv.shape[2]
    heads = hcols // HEAD_DIM
    C, NH = (CHUNKS, HALVES)
    cr = rows // C
    qc = T * cr
    NP = DP * S
    assert TOK_FRAME % rows == 0 and S * fr_dev <= LANES and DP == 2
    vm = pl.BlockSpec(memory_space=pltpu.VMEM)
    hbm = pl.BlockSpec(memory_space=pl.ANY)
    dma = pltpu.SemaphoreType.DMA
    frames = S * fr_dev
    hidden, small = pl.pallas_call(
        kernel,
        out_shape=(
            jax.ShapeDtypeStruct((C, cr, width), BF16),
            jax.ShapeDtypeStruct((2 * DP, frames, LANES), F32),
        ),
        in_specs=[hbm] * 10 + [pl.BlockSpec(memory_space=pltpu.SMEM)],
        out_specs=(vm, vm),
        scratch_shapes=[
            pltpu.VMEM((C, cr, width), BF16),
            pltpu.VMEM((1, width), F32),
            pltpu.VMEM((1, width), F32),
            pltpu.VMEM((chunks, LANES), F32),
            pltpu.VMEM((chunks, LANES), F32),
            pltpu.VMEM((chunks, LANES), F32),
            pltpu.VMEM(w_qkv.shape, BF16),
            pltpu.VMEM((T, NP, hcols // NP, width), BF16),
            pltpu.VMEM(w_up.shape, BF16),
            pltpu.VMEM(w_down.shape, BF16),
            pltpu.VMEM((T, C, cr, width), BF16),
            pltpu.VMEM((T, C, cr, hcols), BF16),
            pltpu.VMEM((S, T, NH, 2, rows // NH, hcols), BF16),
            pltpu.VMEM((heads, 1, qc), F32),
            pltpu.VMEM((heads, 1, qc), F32),
            pltpu.VMEM((heads, HEAD_DIM, qc), F32),
            pltpu.VMEM((C, T, qc, hcols), BF16),
            pltpu.VMEM((T, cr, width), BF16),
            pltpu.VMEM((C, cr, width), F32),
            pltpu.VMEM((qc, width), BF16),
            pltpu.VMEM((qc, w_up.shape[1]), BF16),
            pltpu.VMEM((C, T, cr, width), BF16),
            pltpu.VMEM((C, 2, T, cr, width), BF16),
            pltpu.VMEM((T, chunks, LANES), F32),
            pltpu.VMEM((DP, S, fr_dev, chunks, LANES), F32),
            pltpu.VMEM((DP, frames, LANES), F32),
            dma((10,)),
            dma((2, T)),
            dma((T, NH)),
            dma((S,)),
            dma((T * NH * 2 + S,)),
            dma((1,)),
            dma((2, T)),
            dma((S,)),
            dma((2,)),
            dma((1,)),
            dma((T, S, 2)),
            dma((1,)),
            dma((2, T)),
            dma((C, T)),
            dma((2, T)),
            dma((2, C, T, PIECES)),
            dma((T,)),
            dma((T,)),
            dma((DP * S,)),
            dma((DP, S)),
        ],
        compiler_params=pltpu.CompilerParams(
            collective_id=0, has_side_effects=True, vmem_limit_bytes=67043328
        ),
    )(
        tokens.reshape(C, cr, width),
        attn_gain[None],
        w_qkv,
        w_out.reshape(NP, hcols // NP, width),
        mlp_gain[None],
        w_up,
        w_down,
        pool_gain.reshape(chunks, LANES),
        pool_bias.reshape(chunks, LANES),
        value_weight.reshape(chunks, LANES),
        valid_frames,
    )
    roll, seq = (lax.axis_index("dp"), lax.axis_index("seq"))
    values = lax.dynamic_slice(small, (roll, seq * fr_dev, 0), (1, fr_dev, 1))[..., 0]
    advantages = lax.dynamic_slice(small, (DP + roll, seq * fr_dev, 0), (1, fr_dev, 1))[..., 0]
    return (hidden.reshape(1, rows, width), values, advantages)


def solution(mesh):
    in_specs = (
        P("dp", ("seq", "tensor"), None),
        P(),
        P(None, None, "tensor"),
        P("tensor", None),
        P(),
        P(None, "tensor"),
        P("tensor", None),
        P(),
        P(),
        P(),
        P(),
    )
    out_specs = (P("dp", ("seq", "tensor"), None), P("dp", "seq"), P("dp", "seq"))
    return jax.shard_map(local, mesh=mesh, in_specs=in_specs, out_specs=out_specs, check_vma=False)
```
